32 devices in a mesh: row: 8 (over z, y), col: 4 (over x, core).
Axes of the slice: x: 2, y: 2, z: 4, core: 2. Of those that a mesh axis runs over, the one named last changes fastest.
Arguments:
- moment: bfloat16 [2, 4096, 4096], P(None, 'row', 'col'), may hold values from -6 to 6
- second: float32 [2, 4096, 4096], P(None, 'row', 'col'), may hold values from 0.04 to 2
- left_old: bfloat16 [2, 4096, 4096], P(None, 'col', 'row'), may hold values from -0.09375 to 0.09375
- left_new: bfloat16 [2, 4096, 4096], P(None, 'col', 'row'), may hold values from -0.09375 to 0.09375
- right_old: bfloat16 [4096, 4096], P('row', 'col'), may hold values from -0.09375 to 0.09375
- right_new: bfloat16 [4096, 4096], P('row', 'col'), may hold values from -0.09375 to 0.09375
Outputs:
- moment_new: bfloat16 [2, 4096, 4096], P(None, 'row', 'col')
- direction: bfloat16 [2, 4096, 4096], P(None, 'row', 'col')
The draws below stay inside these ranges and needn't reach their ends.
All inputs are finite; a program needn't handle non-finite values.
Results may differ from the reference program's by a relative error of at most 0.03.
Values may be sent and summed in bfloat16 or wider, within the bound.
A program may use at most 128 MiB of HBM per device.

```python
import math
import jax
import jax.numpy as jnp
from jax import lax

LBLK = 4096
RW = 4096
NBLK = 2
N_ROW = 8
N_COL = 4


def levels(own_key, dims, cuts, low, top_value):
    factor_of = 1.0
    for dim, parts in cuts:
        steps = jax.random.uniform(jax.random.fold_in(jax.random.fold_in(own_key, 6), dim), (parts,), jnp.float32, low / len(cuts), top_value / len(cuts))
        factor_of = factor_of * jnp.repeat(jnp.exp(steps), dims[dim] // parts).reshape((-1,) + (1,) * (len(dims) - 1 - dim))
    return factor_of


def gaussian(stream_key, dims, width, reach, split=(), kind=jnp.bfloat16):
    array = width * jax.random.normal(stream_key, dims, jnp.float32)
    if split:
        array = array * levels(stream_key, dims, split, -0.22, 0.18)
    return jnp.clip(array, -reach, reach).astype(kind)


def setup_inputs(seed: int = 0) -> dict:
    streams_of = jax.random.split(jax.random.key(seed), 7)
    return {
        "moment": gaussian(streams_of[0], (NBLK, LBLK, RW), 1.0, 6.0, ((1, 8), (2, 4))),
        "second": jnp.clip(jnp.exp(math.log(2.0) - 3.912023 * jax.random.uniform(streams_of[1], (NBLK, LBLK, RW), jnp.float32) ** levels(streams_of[1], (NBLK, LBLK, RW), ((1, 8), (2, 4)), -0.2, 0.2)), 0.04, 2.0),
        "left_old": gaussian(streams_of[2], (NBLK, LBLK, LBLK), LBLK ** -0.5, 0.09375, ((1, 4), (2, 8))),
        "left_new": gaussian(streams_of[3], (NBLK, LBLK, LBLK), LBLK ** -0.5, 0.09375, ((1, 4), (2, 8))),
        "right_old": gaussian(streams_of[4], (RW, RW), RW ** -0.5, 0.09375, ((0, 8), (1, 4))),
        "right_new": gaussian(streams_of[5], (RW, RW), RW ** -0.5, 0.09375, ((0, 8), (1, 4))),
    }


def grouped_product(new_basis, old_basis, groups):
    group_rows = new_basis.shape[0] // groups

    def accumulate(running, group_index):
        offset = (group_index * group_rows).astype(jnp.int32)
        new_part = lax.dynamic_slice_in_dim(new_basis, offset, group_rows, 0)
        old_part = lax.dynamic_slice_in_dim(old_basis, offset, group_rows, 0)
        partial_sum = jnp.dot(new_part.T, old_part, preferred_element_type=jnp.float32)
        rounded = lax.optimization_barrier(partial_sum.astype(jnp.bfloat16))
        return (running + rounded.astype(jnp.float32), None)
    start_sum = jnp.zeros((new_basis.shape[1], old_basis.shape[1]), jnp.float32)
    running, unused = lax.scan(accumulate, start_sum, jnp.arange(groups, dtype=jnp.int32))
    return running.astype(jnp.bfloat16)

def reference(moment, second, left_old, left_new, right_old, right_new):
    right_transition = grouped_product(right_new, right_old, N_ROW)

    def one_block(inputs):
        block_moment, block_old, block_new = inputs
        left_transition = grouped_product(block_new, block_old, N_COL)
        rotated = jnp.dot(left_transition, block_moment, preferred_element_type=jnp.float32).astype(jnp.bfloat16)
        return jnp.dot(rotated, right_transition.T, preferred_element_type=jnp.float32).astype(jnp.bfloat16)
    moment_new = lax.map(one_block, (moment, left_old, left_new))
    direction = (moment_new.astype(jnp.float32) / (jnp.sqrt(second) + 1e-08)).astype(jnp.bfloat16)
    return (moment_new, direction)
```

```python
import jax
import jax.numpy as jnp
from jax import lax
from jax.sharding import PartitionSpec as P

F32 = jnp.float32
BF16 = jnp.bfloat16
R_CHUNKS = 2


def add(a, b):
    return (a.astype(F32) + b.astype(F32)).astype(BF16)


def dot_tn(a, b):
    return lax.dot_general(a, b, (((0,), (0,)), ((), ())), preferred_element_type=F32)


def make_local(n_row, n_col):
    nz = n_row // 2
    bits = [1 << s for s in range(n_col.bit_length() - 1)]

    def row_send(value, pairs):
        return lax.ppermute(value, "row", [(z * 2 + y, t * 2 + (y ^ f)) for z, t, f in pairs for y in range(2)])

    def over_y(value):
        return row_send(value, [(z, z, 1) for z in range(nz)])

    def over_pair(value):
        return row_send(value, [(z, z ^ 1, 0) for z in range(nz)])

    def over_class(value, d):
        return row_send(value, [(z, (z + 2 * d) % nz, 0) for z in range(nz)])

    def over_col(value, bit):
        return lax.ppermute(value, "col", [(c, c ^ bit) for c in range(n_col)])

    def gather_col(value):
        chunks = {0: value}
        for bit in reversed(bits):
            for j in list(chunks):
                chunks[j ^ bit] = over_col(chunks[j], bit)
        return chunks

    def local(moment, second, left_old, left_new, right_old, right_new):
        y = lax.axis_index("row") % 2
        z = lax.axis_index("row") // 2
        c = lax.axis_index("col") % 2

        def block(value, index):
            return lax.dynamic_index_in_dim(value, index, 0, keepdims=False)

        old = [block(left_old, y), over_y(block(left_old, 1 - y))]
        new = [block(left_new, y), over_y(block(left_new, 1 - y))]
        rn = jnp.concatenate([right_new, over_y(right_new)], axis=0)
        half = right_old.shape[1] // 2
        ro = jnp.concatenate(
            [
                lax.dynamic_slice_in_dim(right_old, y * half, half, 1),
                over_y(lax.dynamic_slice_in_dim(right_old, (1 - y) * half, half, 1)),
            ],
            axis=0,
        )
        mom = [block(moment, y), over_y(block(moment, 1 - y))]

        far_old = [[over_class(v, d) for v in old] for d in range(1, nz // 2)]
        pair_new = jnp.concatenate(new + [over_pair(v) for v in new], axis=1)
        far_mom = [[over_class(v, d) for v in mom] for d in range(1, nz // 2)]

        ro_all = gather_col(ro)
        right = jnp.concatenate([dot_tn(ro_all[j], rn).astype(BF16) for j in range(n_col)], axis=0)
        parts = jnp.split(right, R_CHUNKS, axis=0)
        h = nz // 2
        for s in range(h - 1):
            pairs = [(s, s + 1, 0), (nz - 1 - s, nz - 2 - s, 0)]
            parts = [add(v, row_send(v, pairs)) for v in parts]
        parts = [add(v, row_send(v, [(h - 1, h, 0), (h, h - 1, 0)])) for v in parts]
        for s in reversed(range(h - 1)):
            pairs = [(s + 1, s, 0), (nz - 2 - s, nz - 1 - s, 0)]
            end = (z == s) | (z == nz - 1 - s)
            parts = [jnp.where(end, row_send(v, pairs), v) for v in parts]
        mine = jnp.concatenate(parts, axis=0).reshape(n_col, half, -1)
        theirs = jnp.concatenate([over_y(v) for v in parts], axis=0).reshape(n_col, half, -1)
        right = jnp.concatenate([jnp.where(y == 0, mine, theirs), jnp.where(y == 0, theirs, mine)], axis=1)

        def panel(cols):
            partial = dot_tn(pair_new, jnp.concatenate(cols, axis=1)).astype(BF16)
            rows = partial.shape[0] // 2
            sent = lax.dynamic_slice_in_dim(partial, (1 - c) * rows, rows, 0)
            kept = lax.dynamic_slice_in_dim(partial, c * rows, rows, 0)
            total = add(kept, over_col(sent, 1))
            for bit in bits[1:]:
                total = add(total, over_col(total, bit))
            across = over_col(total, 1)
            return jnp.where(c == 0, total, across), jnp.where(c == 0, across, total)

        panels = [panel(cols) for cols in [old] + far_old]
        moms = [jnp.concatenate(rows, axis=0) for rows in [mom] + far_mom]

        def rotate(which):
            total = None
            for pan, rows in zip(panels, moms):
                term = jnp.dot(pan[which], rows, preferred_element_type=F32)
                total = term if total is None else total + term
            return total

        back = over_pair(rotate(1).astype(BF16))
        rotated = (rotate(0) + back.astype(F32)).astype(BF16)

        total = None
        for j, chunk in gather_col(rotated).items():
            term = jnp.dot(chunk, right[j], preferred_element_type=F32)
            total = term if total is None else total + term
        out = total.astype(BF16)
        rows = out.shape[0] // 2
        own, other = out[:rows], over_y(out[rows:])
        moment_new = jnp.where(y == 0, jnp.stack([own, other]), jnp.stack([other, own]))
        direction = (moment_new.astype(F32) / (jnp.sqrt(second) + 1e-08)).astype(BF16)
        return moment_new, direction

    return local


def solution(mesh):
    spec = P(None, "row", "col")
    return jax.shard_map(
        make_local(mesh.shape["row"], mesh.shape["col"]),
        mesh=mesh,
        in_specs=(spec, spec, P(None, "col", "row"), P(None, "col", "row"), P("row", "col"), P("row", "col")),
        out_specs=(spec, spec),
        check_vma=False,
    )
```

```python
import functools

import jax
import jax.numpy as jnp
from jax import lax
from jax.experimental import pallas as pl
from jax.experimental.pallas import tpu as pltpu
from jax.sharding import PartitionSpec as P

F32 = jnp.float32
BF16 = jnp.bfloat16
MESH = pl.DeviceIdType.MESH


def dot_tn(a, b):
    return lax.dot_general(a, b, (((0,), (0,)), ((), ())), preferred_element_type=F32)


def dot(a, b):
    return jnp.dot(a, b, preferred_element_type=F32)


class Sizes:
    def __init__(self, n_row, n_col, left_shape, right_shape):
        self.nz, self.nx, self.nc = n_row // 2, n_col // 2, n_col
        self.classes = self.nz // 2
        self.group = self.classes // 2
        _, self.w, self.j = left_shape
        self.q, self.k = right_shape
        self.half = self.k // 2
        self.pc = 128
        self.chunks = self.k // self.pc
        self.kc = 2
        self.kw = self.k // self.kc
        self.cols = self.group * 2 * self.j
        self.tile = min(256, self.j)


def kernel(s, mom, lo, ln, ro, rn, mo, yold, ro_all, fold_in, new, old, mm, rnv, ros, rp, cross, right, left, xrecv, buf, rot_in, rot_all, stage, ssem, rsem, lsem):
    row, col = lax.axis_index("row"), lax.axis_index("col")
    y, z = lax.rem(row, 2), lax.div(row, 2)
    c, x = lax.rem(col, 2), lax.div(col, 2)
    yp, cp = 1 - y, 1 - c
    zp = z + 1 - 2 * lax.rem(z, 2)
    depth = jnp.minimum(z, s.nz - 1 - z)
    upper = z >= s.nz // 2
    inner = jnp.where(upper, z - 1, z + 1)
    outer = jnp.where(upper, z + 1, z - 1)
    is_mid = depth == s.nz // 2 - 1
    is_end = depth == 0
    count = [0, 0]
    drains = []

    def where_is(zz, yy, xx, cc):
        return (zz * 2 + yy, xx * 2 + cc)

    def fresh(n=1):
        count[0] += n
        return count[0] - n

    def remote(src, dst, target, sem):
        return pltpu.make_async_remote_copy(
            src_ref=src, dst_ref=dst, send_sem=ssem.at[sem], recv_sem=rsem.at[sem], device_id=target, device_id_type=MESH
        )

    def begin(copy, pred=None, drain=True):
        if pred is None:
            copy.start()
        else:
            pl.when(pred)(copy.start)
        if drain:
            drains.append((copy, pred))

    def recv(copy, pred=None):
        if pred is None:
            copy.wait_recv()
        else:
            pl.when(pred)(copy.wait_recv)

    def sent(copy, pred=None):
        if pred is None:
            copy.wait_send()
        else:
            pl.when(pred)(copy.wait_send)

    def load(src, dst, pred=None):
        count[1] += 1
        copy = pltpu.make_async_copy(src, dst, lsem.at[count[1] - 1])
        if pred is None:
            copy.start()
        else:
            pl.when(pred)(copy.start)
        return copy, pred

    def done(item):
        copy, pred = item
        if pred is None:
            copy.wait()
        else:
            pl.when(pred)(copy.wait)

    near_y = where_is(z, yp, x, c)
    near_c = where_is(z, y, x, cp)
    near_z = where_is(zp, y, x, c)

    def at_class(d, core):
        return where_is(lax.rem(z - 2 * d + s.nz, s.nz), y, x, core)

    def at_x(d):
        return where_is(z, y, lax.rem(x + d, s.nx), c)

    def col_from(d):
        return lax.rem(x - d + s.nx, s.nx) * 2 + c

    own_half = pl.ds(pl.multiple_of(y * s.half, s.half), s.half)
    other_half = pl.ds(pl.multiple_of(yp * s.half, s.half), s.half)

    y_ro = remote(ro.at[:, other_half], ro_all.at[col, 1], near_y, fresh())
    y_rn = remote(rn, rnv.at[1], near_y, fresh())
    y_old = remote(lo.at[yp], yold, near_y, fresh())
    y_new = remote(ln.at[yp], new.at[c, 1], near_y, fresh())
    y_mom = [remote(mom.at[yp, :, pl.ds(k * s.kw, s.kw)], mm.at[0, 1, :, pl.ds(k * s.kw, s.kw)], near_y, fresh()) for k in range(s.kc)]

    old_sems = {(d, p): fresh(2) for d in range(s.classes) for p in range(2)}

    def old_copy(d, p, who):
        src = lo.at[y] if p == 0 else yold
        return remote(src, old.at[who, d % s.group, p], at_class(d, d // s.group), old_sems[d, p] + who)

    new_z = [remote(ln.at[y] if p == 0 else new.at[c, 1], new.at[c, 2 + p], near_z, fresh()) for p in range(2)]
    new_c = [remote(ln.at[y] if p == 0 else new.at[c, p], new.at[c, p], near_c, fresh()) for p in range(4)]

    def mom_src(p, k):
        part = pl.ds(k * s.kw, s.kw)
        return mom.at[y, :, part] if p == 0 else mm.at[0, 1, :, part]

    mom_z = {
        (d, p, k): remote(mom_src(p, k), mm.at[d, p, :, pl.ds(k * s.kw, s.kw)], at_class(d, c), fresh())
        for d in range(1, s.classes) for p in range(2) for k in range(s.kc)
    }
    ro_src = [ro.at[:, own_half], ro_all.at[col, 1]]
    ro_c = {(0, p): remote(ro_src[p], ro_all.at[col, p], near_c, fresh()) for p in range(2)}
    ro_x = {(d, p): remote(ro_src[p], ro_all.at[col, p], at_x(d), fresh()) for d in range(1, s.nx) for p in range(2)}
    for d in range(1, s.nx):
        for p in range(2):
            ro_c[d, p] = remote(ro_all.at[col_from(d), p], ro_all.at[col_from(d), p], near_c, fresh())

    loads_new = load(ln.at[y], new.at[c, 0])
    loads_old = [load(lo.at[y], old.at[0, 0, 0], c == 0)]
    loads_rn = load(rn, rnv.at[0])
    loads_mom = load(mom.at[y], mm.at[0, 0])

    begin(y_ro)
    begin(y_rn)
    begin(y_old)
    begin(y_new)
    for item in y_mom:
        begin(item)

    def old_send(d, p):
        if d == 0:
            begin(old_copy(0, p, 1), c == 1)
        else:
            begin(old_copy(d, p, c))

    for d in range(1, s.classes):
        old_send(d, 0)
    begin(new_z[0])
    begin(ro_c[0, 0])
    for d in range(1, s.nx):
        begin(ro_x[d, 0])
    begin(new_c[0])
    old_send(0, 0)
    for d in range(1, s.classes):
        begin(mom_z[d, 0, 0])

    recv(y_ro)
    begin(ro_c[0, 1])
    for d in range(1, s.nx):
        begin(ro_x[d, 1])
    for d in range(1, s.nx):
        for p in range(2):
            recv(ro_x[d, p])
            begin(ro_c[d, p])
    recv(y_old)
    for d in range(1, s.classes):
        old_send(d, 1)
    old_send(0, 1)
    loads_old.append(load(yold, old.at[0, 0, 1], c == 0))
    recv(y_rn)
    done(loads_rn)
    for d in range(s.nx):
        for p in range(2):
            recv(ro_c[d, p])

    steps = s.half // s.tile

    def right_piece(i, _):
        mine = i == col
        head = pltpu.make_async_copy(ro.at[:, own_half], ros.at[0], stage_sem(0))
        head_far = pltpu.make_async_copy(ro_all.at[i, 0], ros.at[0], stage_sem(0))
        tail = pltpu.make_async_copy(ro_all.at[i, 1], ros.at[1], stage_sem(1))
        pl.when(mine)(head.start)
        pl.when(jnp.logical_not(mine))(head_far.start)
        tail.start()
        head.wait()
        tail.wait()

        for t in range(steps):
            part = pl.ds(t * s.tile, s.tile)
            value = dot_tn(ros[0, :, part], rnv[0]) + dot_tn(ros[1, :, part], rnv[1])
            value = value.astype(BF16)
            rows = pl.ds(pl.multiple_of(i * s.half + t * s.tile, s.tile), s.tile)
            for n in range(s.chunks):
                rp[n, rows, :] = value[:, n * s.pc:(n + 1) * s.pc]
        return 0

    def stage_sem(n):
        return lsem.at[lsem.shape[0] - 1 - n]

    lax.fori_loop(0, s.nc, right_piece, 0)

    fold_send = [remote(rp.at[n], fold_in.at[n], where_is(inner, y, x, c), fresh()) for n in range(s.chunks)]
    cross_send = [remote(rp.at[n], cross.at[n], where_is(inner, y, x, c), fresh()) for n in range(s.chunks)]
    out_send = [remote(right.at[n, y], right.at[n, y], where_is(outer, y, x, c), fresh()) for n in range(s.chunks)]
    right_y = [remote(right.at[n, y], right.at[n, y], near_y, fresh()) for n in range(s.chunks)]
    total_rows = s.nc * s.half
    part_rows = min(256, total_rows)

    def over_rows(fn):
        def step(i, _):
            fn(pl.ds(pl.multiple_of(i * part_rows, part_rows), part_rows))
            return 0
        lax.fori_loop(0, total_rows // part_rows, step, 0)

    def fold(n):
        @pl.when(jnp.logical_not(is_end))
        def _():
            fold_send[n].wait_recv()
            copy = pltpu.make_async_copy(fold_in.at[n], stage, stage_sem(0))
            copy.start()
            copy.wait()

            def step(rows):
                rp[n, rows, :] = (rp[n, rows, :].astype(F32) + stage[rows, :].astype(F32)).astype(BF16)
            over_rows(step)

        begin(fold_send[n], jnp.logical_not(is_mid))
        begin(cross_send[n], is_mid)

    def spread(n):
        @pl.when(is_mid)
        def _():
            cross_send[n].wait_recv()

            def step(rows):
                right[n, y, rows, :] = (rp[n, rows, :].astype(F32) + cross[n, rows, :].astype(F32)).astype(BF16)
            over_rows(step)

        recv(out_send[n], jnp.logical_not(is_mid))
        begin(out_send[n], jnp.logical_not(is_end))
        begin(right_y[n])

    def fold_end(n):
        begin(fold_send[n], is_end)

    folds = [0]

    def fold_upto(n):
        while folds[0] < min(n, s.chunks):
            fold(folds[0])
            folds[0] += 1

    spreads = [0]

    def spread_upto(n):
        while spreads[0] < min(n, s.chunks):
            spread(spreads[0])
            spreads[0] += 1

    recv(y_new)
    begin(new_z[1])
    begin(new_c[1])
    for d in range(1, s.classes):
        for k in range(1, s.kc):
            begin(mom_z[d, 0, k])
    for k in range(s.kc):
        recv(y_mom[k])
        for d in range(1, s.classes):
            begin(mom_z[d, 1, k])

    def left_rows(h):
        def step(t, _):
            per = s.j // s.tile
            piece = 2 * h + lax.div(t, per)
            lanes = pl.ds(pl.multiple_of(lax.rem(t, per) * s.tile, s.tile), s.tile)
            rows = pl.ds(pl.multiple_of(t * s.tile, s.tile), s.tile)
            first = jnp.transpose(new[0, piece, :, lanes])
            second = jnp.transpose(new[1, piece, :, lanes])
            for d in range(s.group):
                for p in range(2):
                    value = dot(first, old[0, d, p]) + dot(second, old[1, d, p])
                    left[c, h, rows, pl.ds((d * 2 + p) * s.j, s.j)] = value.astype(BF16)
            return 0
        lax.fori_loop(0, 2 * s.j // s.tile, step, 0)

    left_x = {(d, h): remote(left.at[c, h], xrecv.at[d - 1, h], at_x(d), fresh()) for d in range(1, s.nx) for h in range(2)}
    left_c = [remote(left.at[c, h], left.at[c, h], near_c, fresh()) for h in range(2)]

    done(loads_new)
    for p in range(2):
        recv(new_c[p])
    for d in range(s.classes):
        for p in range(2):
            g = d // s.group
            for who in range(2):
                if d == 0 and who == 0:
                    done(loads_old[p])
                else:
                    recv(old_copy(d, p, who), c == g)
    left_rows(0)
    for d in range(1, s.nx):
        begin(left_x[d, 0], drain=False)
    for p in range(2):
        recv(new_z[p])
        begin(new_c[2 + p])
    for p in range(2):
        recv(new_c[2 + p])
    left_rows(1)
    for d in range(1, s.nx):
        begin(left_x[d, 1], drain=False)

    fold_upto(s.chunks // 2)

    rows2 = 2 * s.j

    def left_total(h):
        for d in range(1, s.nx):
            left_x[d, h].wait()

        def step(i, _):
            rows = pl.ds(pl.multiple_of(i * s.tile, s.tile), s.tile)
            value = left[c, h, rows, :].astype(F32)
            for d in range(1, s.nx):
                value = value + xrecv[d - 1, h, rows, :].astype(F32)
            left[c, h, rows, :] = value.astype(BF16)
            return 0
        lax.fori_loop(0, rows2 // s.tile, step, 0)
        begin(left_c[h])

    left_total(0)
    left_total(1)
    spread_upto(s.chunks // 4)
    for h in range(2):
        recv(left_c[h])

    rot_z = [remote(buf.at[:, pl.ds(k * s.kw, s.kw)], rot_in.at[:, pl.ds(k * s.kw, s.kw)], near_z, fresh()) for k in range(s.kc)]

    def rot_part(cc, k):
        return rot_all.at[cc, :, pl.ds(k * s.kw, s.kw)]

    rot_c = {(0, k): remote(rot_part(col, k), rot_part(col, k), near_c, fresh()) for k in range(s.kc)}
    rot_x = {}
    for d in range(1, s.nx):
        for k in range(s.kc):
            rot_x[d, k] = remote(rot_part(col, k), rot_part(col, k), at_x(d), fresh())
            rot_c[d, k] = remote(rot_part(col_from(d), k), rot_part(col_from(d), k), near_c, fresh())

    def rotate(h, k, put):
        part = pl.ds(k * s.kw, s.kw)

        def step(i, _):
            rows = pl.ds(pl.multiple_of(i * s.tile, s.tile), s.tile)
            value = None
            for g in range(2):
                for d in range(s.group):
                    for p in range(2):
                        term = dot(left[g, h, rows, pl.ds((d * 2 + p) * s.j, s.j)], mm[g * s.group + d, p, :, part])
                        value = term if value is None else value + term
            put(rows, part, value)
            return 0
        lax.fori_loop(0, rows2 // s.tile, step, 0)

    def put_far(rows, part, value):
        buf[rows, part] = value.astype(BF16)

    def put_own(rows, part, value):
        rot_all[col, rows, part] = value.astype(BF16)

    done(loads_mom)
    for k in range(s.kc):
        for p in range(2):
            for d in range(1, s.classes):
                recv(mom_z[d, p, k])
        rotate(1, k, put_far)
        begin(rot_z[k], drain=False)
        rotate(0, k, put_own)
    fold_upto(s.chunks)
    for k in range(s.kc):
        part = pl.ds(k * s.kw, s.kw)
        rot_z[k].wait()

        def step(i, _):
            rows = pl.ds(pl.multiple_of(i * s.tile, s.tile), s.tile)
            rot_all[col, rows, part] = (rot_all[col, rows, part].astype(F32) + rot_in[rows, part].astype(F32)).astype(BF16)
            return 0
        lax.fori_loop(0, rows2 // s.tile, step, 0)
        begin(rot_c[0, k])
        for d in range(1, s.nx):
            begin(rot_x[d, k])
    spread_upto(s.chunks // 2)
    for k in range(s.kc):
        for d in range(1, s.nx):
            recv(rot_x[d, k])
            begin(rot_c[d, k])
    for k in range(s.kc):
        for d in range(s.nx):
            recv(rot_c[d, k])

    def product(n):
        lanes = pl.ds(n * s.pc, s.pc)

        def step(i, _):
            rows = pl.ds(pl.multiple_of(i * s.tile, s.tile), s.tile)
            value = None
            for piece in range(s.nc):
                for h in range(2):
                    term = dot(rot_all[piece, rows, pl.ds(h * s.half, s.half)], right[n, h, pl.ds(piece * s.half, s.half), :])
                    value = term if value is None else value + term
            buf[rows, lanes] = value.astype(BF16)
            return 0
        lax.fori_loop(0, rows2 // s.tile, step, 0)
        far = remote(buf.at[pl.ds(s.j, s.j), lanes], mo.at[y, :, lanes], near_y, fresh())
        begin(far)
        return far, load(buf.at[pl.ds(0, s.j), lanes], mo.at[y, :, lanes])

    last = []
    for n in range(s.chunks):
        spread_upto(n + 1 if n + 1 > s.chunks // 2 else s.chunks // 2)
        recv(right_y[n])
        last.append(product(n))
    for far, near in last:
        recv(far)
        done(near)
    for copy, pred in drains:
        sent(copy, pred)
    assert count[0] <= ssem.shape[0] and count[1] <= lsem.shape[0] - 2, count


def make_local(n_row, n_col):
    def local(moment, second, left_old, left_new, right_old, right_new):
        s = Sizes(n_row, n_col, left_old.shape, right_old.shape)
        rows2 = 2 * s.j
        any_spec = pl.BlockSpec(memory_space=pl.ANY)
        n_sems = 40 + 8 * s.chunks + 8 * s.classes * s.kc + 16 * s.nx * s.kc
        flops = 7 * 2 * (rows2 * s.nc * s.k * s.k) // 2
        moment_new, *_ = pl.pallas_call(
            functools.partial(kernel, s),
            out_shape=(
                jax.ShapeDtypeStruct(moment.shape, BF16),
                jax.ShapeDtypeStruct((s.w, s.j), BF16),
                jax.ShapeDtypeStruct((s.nc, 2, s.q, s.half), BF16),
                jax.ShapeDtypeStruct((s.chunks, s.nc * s.half, s.pc), BF16),
            ),
            in_specs=[any_spec] * 5,
            out_specs=(any_spec,) * 4,
            scratch_shapes=[
                pltpu.VMEM((2, 4, s.w, s.j), BF16),
                pltpu.VMEM((2, s.group, 2, s.w, s.j), BF16),
                pltpu.VMEM((s.classes, 2, s.j, s.k), BF16),
                pltpu.VMEM((2, s.q, s.k), BF16),
                pltpu.VMEM((2, s.q, s.half), BF16),
                pltpu.VMEM((s.chunks, s.nc * s.half, s.pc), BF16),
                pltpu.VMEM((s.chunks, s.nc * s.half, s.pc), BF16),
                pltpu.VMEM((s.chunks, 2, s.nc * s.half, s.pc), BF16),
                pltpu.VMEM((2, 2, rows2, s.cols), BF16),
                pltpu.VMEM((max(1, s.nx - 1), 2, rows2, s.cols), BF16),
                pltpu.VMEM((rows2, s.k), BF16),
                pltpu.VMEM((rows2, s.k), BF16),
                pltpu.VMEM((s.nc, rows2, s.k), BF16),
                pltpu.VMEM((s.nc * s.half, s.pc), BF16),
                pltpu.SemaphoreType.DMA((n_sems,)),
                pltpu.SemaphoreType.DMA((n_sems,)),
                pltpu.SemaphoreType.DMA((24,)),
            ],
            compiler_params=pltpu.CompilerParams(has_side_effects=True, vmem_limit_bytes=67043328),
            cost_estimate=pl.CostEstimate(flops=flops, bytes_accessed=2**24, transcendentals=0),
        )(moment, left_old, left_new, right_old, right_new)
        direction = (moment_new.astype(F32) / (jnp.sqrt(second) + 1e-08)).astype(BF16)
        return moment_new, direction

    return local


def solution(mesh):
    spec = P(None, "row", "col")
    return jax.shard_map(
        make_local(mesh.shape["row"], mesh.shape["col"]),
        mesh=mesh,
        in_specs=(spec, spec, P(None, "col", "row"), P(None, "col", "row"), P("row", "col"), P("row", "col")),
        out_specs=(spec, spec),
        check_vma=False,
    )
```

```python
import functools

import jax
import jax.numpy as jnp
from jax import lax
from jax.experimental import pallas as pl
from jax.experimental.pallas import tpu as pltpu
from jax.sharding import PartitionSpec as P

F32 = jnp.float32
BF16 = jnp.bfloat16
MESH = pl.DeviceIdType.MESH


def dot_tn(a, b):
    return lax.dot_general(a, b, (((0,), (0,)), ((), ())), preferred_element_type=F32)


def dot(a, b):
    return jnp.dot(a, b, preferred_element_type=F32)


class Sizes:
    def __init__(self, n_row, n_col, left_shape, right_shape):
        self.nz, self.nx, self.nc = n_row // 2, n_col // 2, n_col
        self.classes = self.nz // 2
        self.group = self.classes // 2
        _, self.w, self.j = left_shape
        self.q, self.k = right_shape
        self.half = self.k // 2
        self.pc = 128
        self.chunks = self.k // self.pc
        self.wide = 2
        self.kc = 2
        self.kw = self.k // self.kc
        self.cols = self.group * 2 * self.j
        self.tile = min(256, self.j)


def kernel(s, mom, lo, ln, ro, rn, mo, yold, ro_all, fold_in, new, old, mm, rnv, ros, rp, cross, right, left, xrecv, buf, rot_in, rot_all, stage, ssem, rsem, lsem):
    row, col = lax.axis_index("row"), lax.axis_index("col")
    y, z = lax.rem(row, 2), lax.div(row, 2)
    c, x = lax.rem(col, 2), lax.div(col, 2)
    yp, cp = 1 - y, 1 - c
    zp = z + 1 - 2 * lax.rem(z, 2)
    depth = jnp.minimum(z, s.nz - 1 - z)
    upper = z >= s.nz // 2
    inner = jnp.where(upper, z - 1, z + 1)
    outer = jnp.where(upper, z + 1, z - 1)
    is_mid = depth == s.nz // 2 - 1
    is_end = depth == 0
    not_mid, not_end = jnp.logical_not(is_mid), jnp.logical_not(is_end)
    between, mid_out = not_mid & not_end, is_mid & not_end
    core0, core1 = c == 0, c == 1
    count = [0, 0]
    drains = {}
    branch = [None]

    def where_is(zz, yy, xx, cc):
        return (zz * 2 + yy, xx * 2 + cc)

    def fresh(n=1):
        count[0] += n
        return count[0] - n

    def remote(src, dst, target, sem):
        return pltpu.make_async_remote_copy(
            src_ref=src, dst_ref=dst, send_sem=ssem.at[sem], recv_sem=rsem.at[sem], device_id=target, device_id_type=MESH
        )

    def begin(copy, pred=None, drain=True):
        if pred is None:
            copy.start()
        else:
            pl.when(pred)(copy.start)
        if drain:
            drains.setdefault(id(copy), (copy, []))[1].append((branch[0], pred))

    def within(pred, fn):
        def run():
            branch[0] = pred
            fn()
            branch[0] = None
        pl.when(pred)(run)

    def recv(copy, pred=None):
        if pred is None:
            copy.wait_recv()
        else:
            pl.when(pred)(copy.wait_recv)

    def sent(copy, pred=None):
        if pred is None:
            copy.wait_send()
        else:
            pl.when(pred)(copy.wait_send)

    def load(src, dst, pred=None):
        count[1] += 1
        copy = pltpu.make_async_copy(src, dst, lsem.at[count[1] - 1])
        if pred is None:
            copy.start()
        else:
            pl.when(pred)(copy.start)
        return copy, pred

    def done(item):
        copy, pred = item
        if pred is None:
            copy.wait()
        else:
            pl.when(pred)(copy.wait)

    near_y = where_is(z, yp, x, c)
    near_c = where_is(z, y, x, cp)
    near_z = where_is(zp, y, x, c)

    def at_class(d, core):
        return where_is(lax.rem(z - 2 * d + s.nz, s.nz), y, x, core)

    def at_x(d):
        return where_is(z, y, lax.rem(x + d, s.nx), c)

    def col_from(d):
        return lax.rem(x - d + s.nx, s.nx) * 2 + c

    own_half = pl.ds(pl.multiple_of(y * s.half, s.half), s.half)
    other_half = pl.ds(pl.multiple_of(yp * s.half, s.half), s.half)

    y_ro = remote(ro.at[:, other_half], ro_all.at[col, 1], near_y, fresh())
    y_rn = remote(rn, rnv.at[1], near_y, fresh())
    y_old = remote(lo.at[yp], yold, near_y, fresh())
    y_new = remote(ln.at[yp], new.at[c, 1], near_y, fresh())
    y_mom = [remote(mom.at[yp, :, pl.ds(k * s.kw, s.kw)], mm.at[0, 1, :, pl.ds(k * s.kw, s.kw)], near_y, fresh()) for k in range(s.kc)]

    old_sems = {(d, p): fresh(2) for d in range(s.classes) for p in range(2)}

    def old_copy(d, p, who):
        src = lo.at[y] if p == 0 else yold
        return remote(src, old.at[who, d % s.group, p], at_class(d, d // s.group), old_sems[d, p] + who)

    old_far = {(d, p): old_copy(d, p, c) for d in range(1, s.classes) for p in range(2)}
    old_near = [old_copy(0, p, 1) for p in range(2)]
    new_z = [remote(ln.at[y] if p == 0 else new.at[c, 1], new.at[c, 2 + p], near_z, fresh()) for p in range(2)]
    new_c = [remote(ln.at[y] if p == 0 else new.at[c, p], new.at[c, p], near_c, fresh()) for p in range(4)]

    def mom_src(p, k):
        part = pl.ds(k * s.kw, s.kw)
        return mom.at[y, :, part] if p == 0 else mm.at[0, 1, :, part]

    mom_z = {
        (d, p, k): remote(mom_src(p, k), mm.at[d, p, :, pl.ds(k * s.kw, s.kw)], at_class(d, c), fresh())
        for d in range(1, s.classes) for p in range(2) for k in range(s.kc)
    }
    ro_src = [ro.at[:, own_half], ro_all.at[col, 1]]
    ro_c = {(0, p): remote(ro_src[p], ro_all.at[col, p], near_c, fresh()) for p in range(2)}
    ro_x = {(d, p): remote(ro_src[p], ro_all.at[col, p], at_x(d), fresh()) for d in range(1, s.nx) for p in range(2)}
    for d in range(1, s.nx):
        for p in range(2):
            ro_c[d, p] = remote(ro_all.at[col_from(d), p], ro_all.at[col_from(d), p], near_c, fresh())

    loads_new = load(ln.at[y], new.at[c, 0])
    loads_old = [load(lo.at[y], old.at[0, 0, 0], c == 0), (pltpu.make_async_copy(yold, old.at[0, 0, 1], lsem.at[lsem.shape[0] - 3]), c == 0)]
    loads_rn = load(rn, rnv.at[0])
    loads_mom = load(mom.at[y], mm.at[0, 0])

    def old_send(d, p):
        if d == 0:
            begin(old_near[p], core1)
        else:
            begin(old_far[d, p])

    def mom_send(p, k, pred=None):
        for d in range(1, s.classes):
            begin(mom_z[d, p, k], pred)

    def step_start():
        begin(y_ro)
        begin(y_rn)
        begin(y_old)
        begin(y_new)
        for item in y_mom:
            begin(item)
        for d in range(1, s.classes):
            old_send(d, 0)
        begin(new_z[0])
        mom_send(0, 0, is_mid)
        begin(ro_c[0, 0])
        for d in range(1, s.nx):
            begin(ro_x[d, 0])
        begin(new_c[0])
        old_send(0, 0)

    def step_right_old():
        recv(y_ro)
        begin(ro_c[0, 1])
        for d in range(1, s.nx):
            begin(ro_x[d, 1])
        for d in range(1, s.nx):
            for p in range(2):
                recv(ro_x[d, p])
                begin(ro_c[d, p])

    steps = s.half // s.tile

    def stage_sem(n):
        return lsem.at[lsem.shape[0] - 1 - n]

    def right_piece(i, _):
        mine = i == col
        head = pltpu.make_async_copy(ro.at[:, own_half], ros.at[0], stage_sem(0))
        head_far = pltpu.make_async_copy(ro_all.at[i, 0], ros.at[0], stage_sem(0))
        tail = pltpu.make_async_copy(ro_all.at[i, 1], ros.at[1], stage_sem(1))
        pl.when(mine)(head.start)
        pl.when(jnp.logical_not(mine))(head_far.start)
        tail.start()
        head.wait()
        tail.wait()

        for t in range(steps):
            part = pl.ds(t * s.tile, s.tile)
            value = dot_tn(ros[0, :, part], rnv[0]) + dot_tn(ros[1, :, part], rnv[1])
            value = value.astype(BF16)
            rows = pl.ds(pl.multiple_of(i * s.half + t * s.tile, s.tile), s.tile)
            for n in range(s.chunks):
                rp[n, rows, :] = value[:, n * s.pc:(n + 1) * s.pc]
        return 0

    def step_right():
        recv(y_rn)
        done(loads_rn)
        for d in range(s.nx):
            for p in range(2):
                recv(ro_c[d, p])
        lax.fori_loop(0, s.nc, right_piece, 0)

    fold_send = [remote(rp.at[n], fold_in.at[n], where_is(inner, y, x, c), fresh()) for n in range(s.chunks)]
    cross_send = [remote(rp.at[n], cross.at[n], where_is(inner, y, x, c), fresh()) for n in range(s.chunks)]
    out_send = [remote(right.at[n, y], right.at[n, y], where_is(outer, y, x, c), fresh()) for n in range(s.chunks)]
    right_y = [remote(right.at[n, y], right.at[n, y], near_y, fresh()) for n in range(s.chunks)]
    total_rows = s.nc * s.half
    part_rows = min(256, total_rows)

    def over_rows(fn):
        def step(i, _):
            fn(pl.ds(pl.multiple_of(i * part_rows, part_rows), part_rows))
            return 0
        lax.fori_loop(0, total_rows // part_rows, step, 0)

    def fold_end(n):
        begin(fold_send[n], is_end)

    def fold(n):
        @pl.when(not_end)
        def _():
            fold_send[n].wait_recv()
            copy = pltpu.make_async_copy(fold_in.at[n], stage, stage_sem(0))
            copy.start()
            copy.wait()

            def step(rows):
                rp[n, rows, :] = (rp[n, rows, :].astype(F32) + stage[rows, :].astype(F32)).astype(BF16)
            over_rows(step)

        begin(fold_send[n], between)
        begin(cross_send[n], is_mid)

    def spread_mid(n):
        @pl.when(is_mid)
        def _():
            cross_send[n].wait_recv()

            def step(rows):
                right[n, y, rows, :] = (rp[n, rows, :].astype(F32) + cross[n, rows, :].astype(F32)).astype(BF16)
            over_rows(step)

        begin(out_send[n], mid_out)
        begin(right_y[n], is_mid)

    def spread_rest(n):
        recv(out_send[n], not_mid)
        begin(out_send[n], between)
        begin(right_y[n], not_mid)

    def step_old():
        recv(y_old)
        for d in range(1, s.classes):
            old_send(d, 1)
        old_send(0, 1)
        loads_old[1][0].start() if loads_old[1][1] is None else pl.when(loads_old[1][1])(loads_old[1][0].start)

    def step_new():
        recv(y_new)
        begin(new_z[1])
        begin(new_c[1])

    def step_mom(k):
        recv(y_mom[k])
        mom_send(1, k)

    per = s.j // s.tile

    def left_rows(piece, p):
        h = piece // 2

        def step(t, _):
            lanes = pl.ds(pl.multiple_of(t * s.tile, s.tile), s.tile)
            rows = pl.ds(pl.multiple_of((piece % 2) * s.j + t * s.tile, s.tile), s.tile)
            first = jnp.transpose(new[0, piece, :, lanes])
            second = jnp.transpose(new[1, piece, :, lanes])
            for d in range(s.group):
                value = dot(first, old[0, d, p]) + dot(second, old[1, d, p])
                left[c, h, rows, pl.ds((p * s.group + d) * s.j, s.j)] = value.astype(BF16)
            return 0
        lax.fori_loop(0, per, step, 0)

    half_cols = s.cols // 2

    def left_part(ref, index, piece, p):
        return ref.at[index, piece // 2, pl.ds((piece % 2) * s.j, s.j), pl.ds(p * half_cols, half_cols)]

    left_units = [(i, p) for p in range(2) for i in (2, 0, 1, 3)]
    left_x = {
        (d,) + u: remote(left_part(left, c, *u), left_part(xrecv, d - 1, *u), at_x(d), fresh())
        for d in range(1, s.nx) for u in left_units
    }
    left_c = {u: remote(left_part(left, c, *u), left_part(left, c, *u), near_c, fresh()) for u in left_units}

    def left_send(piece, p):
        left_rows(piece, p)
        for d in range(1, s.nx):
            begin(left_x[d, piece, p], drain=False)

    def left_first(p):
        for d in range(s.classes):
            g = d // s.group
            for who in range(2):
                if d == 0 and who == 0:
                    done(loads_old[p])
                else:
                    recv(old_copy(d, p, who), c == g)
        for i in (2, 0, 1):
            left_send(i, p)

    def left_total(piece, p):
        for d in range(1, s.nx):
            left_x[d, piece, p].wait()
        lanes = pl.ds(p * half_cols, half_cols)

        def step(t, _):
            rows = pl.ds(pl.multiple_of((piece % 2) * s.j + t * s.tile, s.tile), s.tile)
            value = left[c, piece // 2, rows, lanes].astype(F32)
            for d in range(1, s.nx):
                value = value + xrecv[d - 1, piece // 2, rows, lanes].astype(F32)
            left[c, piece // 2, rows, lanes] = value.astype(BF16)
            return 0
        lax.fori_loop(0, per, step, 0)
        begin(left_c[piece, p])

    rows2 = 2 * s.j
    parts = [(k, h) for k in range(s.kc) for h in (1, 0)]

    def cut(part):
        k, h = part
        return pl.ds(h * s.j, s.j), pl.ds(k * s.kw, s.kw)

    rot_z = {part: remote(buf.at[cut(part)], rot_in.at[cut(part)], near_z, fresh()) for part in parts}

    def rot_part(cc, part):
        return rot_all.at[(cc,) + cut(part)]

    rot_c = {(0, part): remote(rot_part(col, part), rot_part(col, part), near_c, fresh()) for part in parts}
    rot_x = {}
    for d in range(1, s.nx):
        for part in parts:
            rot_x[d, part] = remote(rot_part(col, part), rot_part(col, part), at_x(d), fresh())
            rot_c[d, part] = remote(rot_part(col_from(d), part), rot_part(col_from(d), part), near_c, fresh())

    def over_half(h, fn):
        def step(i, _):
            fn(pl.ds(pl.multiple_of(h * s.j + i * s.tile, s.tile), s.tile))
            return 0
        lax.fori_loop(0, per, step, 0)

    def rotate(h, part, put):
        lanes = cut(part)[1]

        def step(rows):
            value = None
            for g in range(2):
                for d in range(s.group):
                    for p in range(2):
                        term = dot(left[g, h, rows, pl.ds((p * s.group + d) * s.j, s.j)], mm[g * s.group + d, p, :, lanes])
                        value = term if value is None else value + term
            put(rows, lanes, value)
        over_half(part[1], step)

    def put_far(rows, lanes, value):
        buf[rows, lanes] = value.astype(BF16)

    def put_own(rows, lanes, value):
        rot_all[col, rows, lanes] = value.astype(BF16)

    def step_rotate(k):
        for p in range(2):
            for d in range(1, s.classes):
                recv(mom_z[d, p, k])
        for h in (1, 0):
            rotate(1, (k, h), put_far)
            begin(rot_z[k, h], drain=False)

    def step_rotated(part):
        lanes = cut(part)[1]
        rot_z[part].wait()

        def step(rows):
            rot_all[col, rows, lanes] = (rot_all[col, rows, lanes].astype(F32) + rot_in[rows, lanes].astype(F32)).astype(BF16)
        over_half(part[1], step)
        for d in range(1, s.nx):
            begin(rot_x[d, part])
        begin(rot_c[0, part])

    def step_gather(part):
        for d in range(1, s.nx):
            recv(rot_x[d, part])
            begin(rot_c[d, part])

    def product(h, n):
        lanes = pl.ds(n * s.pc, s.wide * s.pc)

        def step(rows):
            value = None
            for piece in range(s.nc):
                for i in range(2):
                    deep = pl.ds(piece * s.half, s.half)
                    columns = jnp.concatenate([right[n + j, i, deep, :] for j in range(s.wide)], axis=1)
                    term = dot(rot_all[piece, rows, pl.ds(i * s.half, s.half)], columns)
                    value = term if value is None else value + term
            buf[rows, lanes] = value.astype(BF16)
        over_half(h, step)
        if h:
            far = remote(buf.at[pl.ds(s.j, s.j), lanes], mo.at[y, :, lanes], near_y, fresh())
            begin(far)
            return far
        return load(buf.at[pl.ds(0, s.j), lanes], mo.at[y, :, lanes])

    def upto(step):
        state = [0]

        def run(n):
            while state[0] < min(n, s.chunks):
                step(state[0])
                state[0] += 1
        return run

    ends, folds, mids, rests = upto(fold_end), upto(fold), upto(spread_mid), upto(spread_rest)
    eighth = max(1, s.chunks // 8)

    def first_part():
        step_start()
        step_right_old()
        step_right()

    def left_ready():
        done(loads_new)
        recv(new_z[0])
        begin(new_c[2])
        for i in range(3):
            recv(new_c[i])

    def left_last():
        recv(new_z[1])
        begin(new_c[3])
        recv(new_c[3])
        for p in range(2):
            left_send(3, p)

    def left_sum(p):
        for i in (2, 0, 1):
            left_total(i, p)

    def left_close():
        for p in range(2):
            left_total(3, p)
        done(loads_mom)
        for u in left_units:
            recv(left_c[u])

    def rotate_own(k):
        for h in (1, 0):
            rotate(0, (k, h), put_own)

    def rotated_all(k):
        for h in (1, 0):
            step_rotated((k, h))

    def gather_all(k):
        for h in (1, 0):
            step_gather((k, h))

    def mom_both(k):
        mom_send(0, k, not_mid if k == 0 else None)
        mom_send(1, k)

    def of(n):
        return max(1, n * s.chunks // 8)

    def middle():
        folds, mids = upto(fold), upto(spread_mid)
        folds(of(2))
        mids(of(1))
        folds(of(3))
        step_new()
        mids(of(2))
        folds(of(4))
        step_old()
        left_ready()
        left_first(0)
        mids(of(3))
        pl.when(core0)(functools.partial(left_first, 1))
        for k in range(s.kc):
            recv(y_mom[k])
        mids(of(4))
        mom_both(0)
        left_sum(0)
        pl.when(core1)(functools.partial(left_first, 1))
        left_last()
        folds(of(6))
        for k in range(1, s.kc):
            mom_both(k)
        left_sum(1)
        left_close()
        step_rotate(0)
        rotate_own(0)
        mids(of(6))
        rotated_all(0)
        folds(s.chunks)
        for k in range(1, s.kc):
            step_rotate(k)
            rotate_own(k)
            gather_all(k - 1)
        mids(s.chunks)
        for k in range(1, s.kc):
            rotated_all(k)
        gather_all(s.kc - 1)

    def others():
        ends, folds, rests = upto(fold_end), upto(fold), upto(spread_rest)
        ends(of(4))
        step_old()
        step_new()
        left_ready()
        left_first(0)
        pl.when(core0)(functools.partial(left_first, 1))
        for k in range(s.kc):
            recv(y_mom[k])
            mom_both(k)
            if k == 0:
                ends(of(6))
        left_sum(0)
        rests(of(2))
        pl.when(core1)(functools.partial(left_first, 1))
        rests(of(4))
        left_last()
        folds(of(6))
        left_sum(1)
        left_close()
        step_rotate(0)
        ends(s.chunks)
        rotate_own(0)
        rotated_all(0)
        rests(of(6))
        folds(s.chunks)
        for k in range(1, s.kc):
            step_rotate(k)
            rotate_own(k)
            gather_all(k - 1)
        for k in range(1, s.kc):
            rotated_all(k)
        rests(s.chunks)
        gather_all(s.kc - 1)

    first_part()
    within(is_mid, middle)
    within(not_mid, others)
    order = [(1, n) for n in range(0, s.chunks - s.wide, s.wide)] + [(0, n) for n in range(0, s.chunks - s.wide, s.wide)]
    order += [(1, s.chunks - s.wide), (0, s.chunks - s.wide)]
    seen = set()
    last = []
    for h, n in order:
        if not seen & {("rows", h)}:
            seen.add(("rows", h))
            for part in parts:
                if part[1] == h:
                    for d in range(s.nx):
                        recv(rot_c[d, part])
        for i in range(s.wide):
            if n + i not in seen:
                seen.add(n + i)
                recv(right_y[n + i])
        item = product(h, n)
        last.append((h, item))
    for h, item in last:
        (recv if h else done)(item)
    for copy, uses in drains.values():
        preds = []
        for pair in uses:
            terms = [term for term in pair if term is not None]
            preds.append(functools.reduce(jnp.logical_and, terms) if terms else None)
        sent(copy, None if any(p is None for p in preds) else functools.reduce(jnp.logical_or, preds))
    assert count[0] <= ssem.shape[0] and count[1] <= lsem.shape[0] - 3, count


def make_local(n_row, n_col):
    def local(moment, second, left_old, left_new, right_old, right_new):
        s = Sizes(n_row, n_col, left_old.shape, right_old.shape)
        rows2 = 2 * s.j
        any_spec = pl.BlockSpec(memory_space=pl.ANY)
        n_sems = 60 + 8 * s.chunks + 8 * s.classes * s.kc + 32 * s.nx * s.kc
        flops = 7 * 2 * (rows2 * s.nc * s.k * s.k) // 2
        moment_new, *_ = pl.pallas_call(
            functools.partial(kernel, s),
            out_shape=(
                jax.ShapeDtypeStruct(moment.shape, BF16),
                jax.ShapeDtypeStruct((s.w, s.j), BF16),
                jax.ShapeDtypeStruct((s.nc, 2, s.q, s.half), BF16),
                jax.ShapeDtypeStruct((s.chunks, s.nc * s.half, s.pc), BF16),
            ),
            in_specs=[any_spec] * 5,
            out_specs=(any_spec,) * 4,
            scratch_shapes=[
                pltpu.VMEM((2, 4, s.w, s.j), BF16),
                pltpu.VMEM((2, s.group, 2, s.w, s.j), BF16),
                pltpu.VMEM((s.classes, 2, s.j, s.k), BF16),
                pltpu.VMEM((2, s.q, s.k), BF16),
                pltpu.VMEM((2, s.q, s.half), BF16),
                pltpu.VMEM((s.chunks, s.nc * s.half, s.pc), BF16),
                pltpu.VMEM((s.chunks, s.nc * s.half, s.pc), BF16),
                pltpu.VMEM((s.chunks, 2, s.nc * s.half, s.pc), BF16),
                pltpu.VMEM((2, 2, rows2, s.cols), BF16),
                pltpu.VMEM((max(1, s.nx - 1), 2, rows2, s.cols), BF16),
                pltpu.VMEM((rows2, s.k), BF16),
                pltpu.VMEM((rows2, s.k), BF16),
                pltpu.VMEM((s.nc, rows2, s.k), BF16),
                pltpu.VMEM((s.nc * s.half, s.pc), BF16),
                pltpu.SemaphoreType.DMA((n_sems,)),
                pltpu.SemaphoreType.DMA((n_sems,)),
                pltpu.SemaphoreType.DMA((24,)),
            ],
            compiler_params=pltpu.CompilerParams(has_side_effects=True, vmem_limit_bytes=67043328),
            cost_estimate=pl.CostEstimate(flops=flops, bytes_accessed=2**24, transcendentals=0),
        )(moment, left_old, left_new, right_old, right_new)
        direction = (moment_new.astype(F32) / (jnp.sqrt(second) + 1e-08)).astype(BF16)
        return moment_new, direction

    return local


def solution(mesh):
    spec = P(None, "row", "col")
    return jax.shard_map(
        make_local(mesh.shape["row"], mesh.shape["col"]),
        mesh=mesh,
        in_specs=(spec, spec, P(None, "col", "row"), P(None, "col", "row"), P("row", "col"), P("row", "col")),
        out_specs=(spec, spec),
        check_vma=False,
    )
```

```python
import functools

import jax
import jax.numpy as jnp
from jax import lax
from jax.experimental import pallas as pl
from jax.experimental.pallas import tpu as pltpu
from jax.sharding import PartitionSpec as P

F32 = jnp.float32
BF16 = jnp.bfloat16
MESH = pl.DeviceIdType.MESH


def dot_tn(a, b):
    return lax.dot_general(a, b, (((0,), (0,)), ((), ())), preferred_element_type=F32)


def dot(a, b):
    return jnp.dot(a, b, preferred_element_type=F32)


class Sizes:
    def __init__(self, n_row, n_col, left_shape, right_shape):
        self.nz, self.nx, self.nc = n_row // 2, n_col // 2, n_col
        self.classes = self.nz // 2
        self.group = self.classes // 2
        _, self.w, self.j = left_shape
        self.q, self.k = right_shape
        self.half = self.k // 2
        self.pc = 128
        self.chunks = self.k // self.pc
        self.wide = 2
        self.kc = 2
        self.kw = self.k // self.kc
        self.cols = self.group * 2 * self.j
        self.tile = min(256, self.j)


def kernel(s, mom, lo, ln, ro, rn, mo, yold, ro_all, fold_in, new, old, mm, rnv, ros, rp, cross, right, left, xrecv, buf, rot_in, rot_all, stage, ssem, rsem, lsem):
    row, col = lax.axis_index("row"), lax.axis_index("col")
    y, z = lax.rem(row, 2), lax.div(row, 2)
    c, x = lax.rem(col, 2), lax.div(col, 2)
    yp, cp = 1 - y, 1 - c
    zp = z + 1 - 2 * lax.rem(z, 2)
    depth = jnp.minimum(z, s.nz - 1 - z)
    upper = z >= s.nz // 2
    inner = jnp.where(upper, z - 1, z + 1)
    outer = jnp.where(upper, z + 1, z - 1)
    is_mid = depth == s.nz // 2 - 1
    is_end = depth == 0
    not_mid, not_end = jnp.logical_not(is_mid), jnp.logical_not(is_end)
    between, mid_out = not_mid & not_end, is_mid & not_end
    core0, core1 = c == 0, c == 1
    count = [0, 0]
    drains = {}
    branch = [None]

    def where_is(zz, yy, xx, cc):
        return (zz * 2 + yy, xx * 2 + cc)

    def fresh(n=1):
        count[0] += n
        return count[0] - n

    def remote(src, dst, target, sem):
        return pltpu.make_async_remote_copy(
            src_ref=src, dst_ref=dst, send_sem=ssem.at[sem], recv_sem=rsem.at[sem], device_id=target, device_id_type=MESH
        )

    def begin(copy, pred=None, drain=True):
        if pred is None:
            copy.start()
        else:
            pl.when(pred)(copy.start)
        if drain:
            drains.setdefault(id(copy), (copy, []))[1].append((branch[0], pred))

    def within(pred, fn):
        def run():
            branch[0] = pred
            fn()
            branch[0] = None
        pl.when(pred)(run)

    def recv(copy, pred=None):
        if pred is None:
            copy.wait_recv()
        else:
            pl.when(pred)(copy.wait_recv)

    def sent(copy, pred=None):
        if pred is None:
            copy.wait_send()
        else:
            pl.when(pred)(copy.wait_send)

    def load(src, dst, pred=None):
        count[1] += 1
        copy = pltpu.make_async_copy(src, dst, lsem.at[count[1] - 1])
        if pred is None:
            copy.start()
        else:
            pl.when(pred)(copy.start)
        return copy, pred

    def done(item):
        copy, pred = item
        if pred is None:
            copy.wait()
        else:
            pl.when(pred)(copy.wait)

    near_y = where_is(z, yp, x, c)
    near_c = where_is(z, y, x, cp)
    near_z = where_is(zp, y, x, c)

    def at_class(d, core):
        return where_is(lax.rem(z - 2 * d + s.nz, s.nz), y, x, core)

    def at_x(d):
        return where_is(z, y, lax.rem(x + d, s.nx), c)

    def col_from(d):
        return lax.rem(x - d + s.nx, s.nx) * 2 + c

    own_half = pl.ds(pl.multiple_of(y * s.half, s.half), s.half)
    other_half = pl.ds(pl.multiple_of(yp * s.half, s.half), s.half)

    loads_new = load(ln.at[y], new.at[c, 0])
    loads_old = [load(lo.at[y], old.at[0, 0, 0], c == 0), (pltpu.make_async_copy(yold, old.at[0, 0, 1], lsem.at[lsem.shape[0] - 3]), c == 0)]
    loads_rn = load(rn, rnv.at[0])
    loads_mom = load(mom.at[y], mm.at[0, 0])

    barrier = pltpu.get_barrier_semaphore()

    def greet(target):
        pl.semaphore_signal(barrier, inc=1, device_id=target, device_id_type=MESH)

    greet(near_y)
    greet(near_c)
    for d in range(1, s.nx):
        greet(at_x(d))
    for d in range(1, s.classes):
        for core in range(2):
            greet(at_class(d, core))
    pl.when(z > 0)(lambda: greet(where_is(z - 1, y, x, c)))
    pl.when(z < s.nz - 1)(lambda: greet(where_is(z + 1, y, x, c)))
    inside = jnp.where((z > 0) & (z < s.nz - 1), 2, 1)
    pl.semaphore_wait(barrier, 2 + s.nx - 1 + 2 * (s.classes - 1) + inside)

    y_ro = remote(ro.at[:, other_half], ro_all.at[col, 1], near_y, fresh())
    y_rn = remote(rn, rnv.at[1], near_y, fresh())
    y_old = remote(lo.at[yp], yold, near_y, fresh())
    y_new = remote(ln.at[yp], new.at[c, 1], near_y, fresh())
    y_mom = [remote(mom.at[yp, :, pl.ds(k * s.kw, s.kw)], mm.at[0, 1, :, pl.ds(k * s.kw, s.kw)], near_y, fresh()) for k in range(s.kc)]

    old_sems = {(d, p): fresh(2) for d in range(s.classes) for p in range(2)}

    def old_copy(d, p, who):
        src = lo.at[y] if p == 0 else yold
        return remote(src, old.at[who, d % s.group, p], at_class(d, d // s.group), old_sems[d, p] + who)

    old_far = {(d, p): old_copy(d, p, c) for d in range(1, s.classes) for p in range(2)}
    old_near = [old_copy(0, p, 1) for p in range(2)]
    new_z = [remote(ln.at[y] if p == 0 else new.at[c, 1], new.at[c, 2 + p], near_z, fresh()) for p in range(2)]
    new_c = [remote(ln.at[y] if p == 0 else new.at[c, p], new.at[c, p], near_c, fresh()) for p in range(4)]

    def mom_src(p, k):
        part = pl.ds(k * s.kw, s.kw)
        return mom.at[y, :, part] if p == 0 else mm.at[0, 1, :, part]

    mom_z = {
        (d, p, k): remote(mom_src(p, k), mm.at[d, p, :, pl.ds(k * s.kw, s.kw)], at_class(d, c), fresh())
        for d in range(1, s.classes) for p in range(2) for k in range(s.kc)
    }
    ro_src = [ro.at[:, own_half], ro_all.at[col, 1]]
    ro_c = {(0, p): remote(ro_src[p], ro_all.at[col, p], near_c, fresh()) for p in range(2)}
    ro_x = {(d, p): remote(ro_src[p], ro_all.at[col, p], at_x(d), fresh()) for d in range(1, s.nx) for p in range(2)}
    for d in range(1, s.nx):
        for p in range(2):
            ro_c[d, p] = remote(ro_all.at[col_from(d), p], ro_all.at[col_from(d), p], near_c, fresh())

    def old_send(d, p):
        if d == 0:
            begin(old_near[p], core1)
        else:
            begin(old_far[d, p])

    def mom_send(p, k, pred=None):
        for d in range(1, s.classes):
            begin(mom_z[d, p, k], pred)

    def step_start():
        begin(y_ro)
        begin(y_rn)
        begin(y_old)
        begin(y_new)
        for item in y_mom:
            begin(item)
        for d in range(1, s.classes):
            old_send(d, 0)
        begin(new_z[0])
        mom_send(0, 0, is_mid)
        begin(ro_c[0, 0])
        for d in range(1, s.nx):
            begin(ro_x[d, 0])
        begin(new_c[0])
        old_send(0, 0)

    def step_right_old():
        recv(y_ro)
        begin(ro_c[0, 1])
        for d in range(1, s.nx):
            begin(ro_x[d, 1])
        for d in range(1, s.nx):
            for p in range(2):
                recv(ro_x[d, p])
                begin(ro_c[d, p])

    steps = s.half // s.tile

    def stage_sem(n):
        return lsem.at[lsem.shape[0] - 1 - n]

    def right_piece(i, _):
        mine = i == col
        head = pltpu.make_async_copy(ro.at[:, own_half], ros.at[0], stage_sem(0))
        head_far = pltpu.make_async_copy(ro_all.at[i, 0], ros.at[0], stage_sem(0))
        tail = pltpu.make_async_copy(ro_all.at[i, 1], ros.at[1], stage_sem(1))
        pl.when(mine)(head.start)
        pl.when(jnp.logical_not(mine))(head_far.start)
        tail.start()
        head.wait()
        tail.wait()

        for t in range(steps):
            part = pl.ds(t * s.tile, s.tile)
            value = dot_tn(ros[0, :, part], rnv[0]) + dot_tn(ros[1, :, part], rnv[1])
            value = value.astype(BF16)
            rows = pl.ds(pl.multiple_of(i * s.half + t * s.tile, s.tile), s.tile)
            for n in range(s.chunks):
                rp[n, rows, :] = value[:, n * s.pc:(n + 1) * s.pc]
        return 0

    def step_right():
        recv(y_rn)
        done(loads_rn)
        for d in range(s.nx):
            for p in range(2):
                recv(ro_c[d, p])
        lax.fori_loop(0, s.nc, right_piece, 0)

    fold_send = [remote(rp.at[n], fold_in.at[n], where_is(inner, y, x, c), fresh()) for n in range(s.chunks)]
    cross_send = [remote(rp.at[n], cross.at[n], where_is(inner, y, x, c), fresh()) for n in range(s.chunks)]
    out_send = [remote(right.at[n, y], right.at[n, y], where_is(outer, y, x, c), fresh()) for n in range(s.chunks)]
    right_y = [remote(right.at[n, y], right.at[n, y], near_y, fresh()) for n in range(s.chunks)]
    total_rows = s.nc * s.half
    part_rows = min(256, total_rows)

    def over_rows(fn):
        def step(i, _):
            fn(pl.ds(pl.multiple_of(i * part_rows, part_rows), part_rows))
            return 0
        lax.fori_loop(0, total_rows // part_rows, step, 0)

    def fold_end(n):
        begin(fold_send[n], is_end)

    def fold(n):
        @pl.when(not_end)
        def _():
            fold_send[n].wait_recv()
            copy = pltpu.make_async_copy(fold_in.at[n], stage, stage_sem(0))
            copy.start()
            copy.wait()

            def step(rows):
                rp[n, rows, :] = (rp[n, rows, :].astype(F32) + stage[rows, :].astype(F32)).astype(BF16)
            over_rows(step)

        begin(fold_send[n], between)
        begin(cross_send[n], is_mid)

    def spread_mid(n):
        @pl.when(is_mid)
        def _():
            cross_send[n].wait_recv()

            def step(rows):
                right[n, y, rows, :] = (rp[n, rows, :].astype(F32) + cross[n, rows, :].astype(F32)).astype(BF16)
            over_rows(step)

        begin(out_send[n], mid_out)
        begin(right_y[n], is_mid)

    def spread_rest(n):
        recv(out_send[n], not_mid)
        begin(out_send[n], between)
        begin(right_y[n], not_mid)

    def step_old():
        recv(y_old)
        for d in range(1, s.classes):
            old_send(d, 1)
        old_send(0, 1)
        loads_old[1][0].start() if loads_old[1][1] is None else pl.when(loads_old[1][1])(loads_old[1][0].start)

    def step_new():
        recv(y_new)
        begin(new_z[1])
        begin(new_c[1])

    def step_mom(k):
        recv(y_mom[k])
        mom_send(1, k)

    per = s.j // s.tile

    def left_rows(piece, p):
        h = piece // 2

        def step(t, _):
            lanes = pl.ds(pl.multiple_of(t * s.tile, s.tile), s.tile)
            rows = pl.ds(pl.multiple_of((piece % 2) * s.j + t * s.tile, s.tile), s.tile)
            first = jnp.transpose(new[0, piece, :, lanes])
            second = jnp.transpose(new[1, piece, :, lanes])
            for d in range(s.group):
                value = dot(first, old[0, d, p]) + dot(second, old[1, d, p])
                left[c, h, rows, pl.ds((p * s.group + d) * s.j, s.j)] = value.astype(BF16)
            return 0
        lax.fori_loop(0, per, step, 0)

    half_cols = s.cols // 2

    def left_part(ref, index, piece, p):
        return ref.at[index, piece // 2, pl.ds((piece % 2) * s.j, s.j), pl.ds(p * half_cols, half_cols)]

    left_units = [(i, p) for p in range(2) for i in (2, 0, 1, 3)]
    left_x = {
        (d,) + u: remote(left_part(left, c, *u), left_part(xrecv, d - 1, *u), at_x(d), fresh())
        for d in range(1, s.nx) for u in left_units
    }
    left_c = {u: remote(left_part(left, c, *u), left_part(left, c, *u), near_c, fresh()) for u in left_units}

    def left_send(piece, p):
        left_rows(piece, p)
        for d in range(1, s.nx):
            begin(left_x[d, piece, p], drain=False)

    def left_first(p):
        for d in range(s.classes):
            g = d // s.group
            for who in range(2):
                if d == 0 and who == 0:
                    done(loads_old[p])
                else:
                    recv(old_copy(d, p, who), c == g)
        for i in (2, 0, 1):
            left_send(i, p)

    def left_total(piece, p):
        for d in range(1, s.nx):
            left_x[d, piece, p].wait()
        lanes = pl.ds(p * half_cols, half_cols)

        def step(t, _):
            rows = pl.ds(pl.multiple_of((piece % 2) * s.j + t * s.tile, s.tile), s.tile)
            value = left[c, piece // 2, rows, lanes].astype(F32)
            for d in range(1, s.nx):
                value = value + xrecv[d - 1, piece // 2, rows, lanes].astype(F32)
            left[c, piece // 2, rows, lanes] = value.astype(BF16)
            return 0
        lax.fori_loop(0, per, step, 0)
        begin(left_c[piece, p])

    rows2 = 2 * s.j
    parts = [(k, h) for k in range(s.kc) for h in (1, 0)]

    def cut(part):
        k, h = part
        return pl.ds(h * s.j, s.j), pl.ds(k * s.kw, s.kw)

    rot_z = {part: remote(buf.at[cut(part)], rot_in.at[cut(part)], near_z, fresh()) for part in parts}

    def rot_part(cc, part):
        return rot_all.at[(cc,) + cut(part)]

    rot_c = {(0, part): remote(rot_part(col, part), rot_part(col, part), near_c, fresh()) for part in parts}
    rot_x = {}
    for d in range(1, s.nx):
        for part in parts:
            rot_x[d, part] = remote(rot_part(col, part), rot_part(col, part), at_x(d), fresh())
            rot_c[d, part] = remote(rot_part(col_from(d), part), rot_part(col_from(d), part), near_c, fresh())

    def over_half(h, fn):
        def step(i, _):
            fn(pl.ds(pl.multiple_of(h * s.j + i * s.tile, s.tile), s.tile))
            return 0
        lax.fori_loop(0, per, step, 0)

    def rotate(h, part, put):
        lanes = cut(part)[1]

        def step(rows):
            value = None
            for g in range(2):
                for d in range(s.group):
                    for p in range(2):
                        term = dot(left[g, h, rows, pl.ds((p * s.group + d) * s.j, s.j)], mm[g * s.group + d, p, :, lanes])
                        value = term if value is None else value + term
            put(rows, lanes, value)
        over_half(part[1], step)

    def put_far(rows, lanes, value):
        buf[rows, lanes] = value.astype(BF16)

    def put_own(rows, lanes, value):
        rot_all[col, rows, lanes] = value.astype(BF16)

    def step_rotate(k):
        for p in range(2):
            for d in range(1, s.classes):
                recv(mom_z[d, p, k])
        for h in (1, 0):
            rotate(1, (k, h), put_far)
            begin(rot_z[k, h], drain=False)

    def step_rotated(part):
        lanes = cut(part)[1]
        rot_z[part].wait()

        def step(rows):
            rot_all[col, rows, lanes] = (rot_all[col, rows, lanes].astype(F32) + rot_in[rows, lanes].astype(F32)).astype(BF16)
        over_half(part[1], step)
        for d in range(1, s.nx):
            begin(rot_x[d, part])
        begin(rot_c[0, part])

    def step_gather(part):
        for d in range(1, s.nx):
            recv(rot_x[d, part])
            begin(rot_c[d, part])

    def product(h, n):
        lanes = pl.ds(n * s.pc, s.wide * s.pc)

        def step(rows):
            value = None
            for piece in range(s.nc):
                for i in range(2):
                    deep = pl.ds(piece * s.half, s.half)
                    columns = jnp.concatenate([right[n + j, i, deep, :] for j in range(s.wide)], axis=1)
                    term = dot(rot_all[piece, rows, pl.ds(i * s.half, s.half)], columns)
                    value = term if value is None else value + term
            buf[rows, lanes] = value.astype(BF16)
        over_half(h, step)
        if h:
            far = remote(buf.at[pl.ds(s.j, s.j), lanes], mo.at[y, :, lanes], near_y, fresh())
            begin(far)
            return far
        return load(buf.at[pl.ds(0, s.j), lanes], mo.at[y, :, lanes])

    def upto(step):
        state = [0]

        def run(n):
            while state[0] < min(n, s.chunks):
                step(state[0])
                state[0] += 1
        return run

    ends, folds, mids, rests = upto(fold_end), upto(fold), upto(spread_mid), upto(spread_rest)
    eighth = max(1, s.chunks // 8)

    def first_part():
        step_start()
        step_right_old()
        step_right()

    def left_ready():
        done(loads_new)
        recv(new_z[0])
        begin(new_c[2])
        for i in range(3):
            recv(new_c[i])

    def left_last():
        recv(new_z[1])
        begin(new_c[3])
        recv(new_c[3])
        for p in range(2):
            left_send(3, p)

    def left_sum(p):
        for i in (2, 0, 1):
            left_total(i, p)

    def left_close():
        for p in range(2):
            left_total(3, p)
        done(loads_mom)
        for u in left_units:
            recv(left_c[u])

    def rotate_own(k):
        for h in (1, 0):
            rotate(0, (k, h), put_own)

    def rotated_all(k):
        for h in (1, 0):
            step_rotated((k, h))

    def gather_all(k):
        for h in (1, 0):
            step_gather((k, h))

    def mom_both(k):
        mom_send(0, k, not_mid if k == 0 else None)
        mom_send(1, k)

    def of(n):
        return max(1, n * s.chunks // 8)

    def middle():
        folds, mids = upto(fold), upto(spread_mid)
        folds(of(2))
        mids(of(1))
        folds(of(3))
        step_new()
        mids(of(2))
        folds(of(4))
        step_old()
        left_ready()
        left_first(0)
        mids(of(3))
        pl.when(core0)(functools.partial(left_first, 1))
        for k in range(s.kc):
            recv(y_mom[k])
        mids(of(4))
        for k in range(s.kc):
            mom_both(k)
        left_sum(0)
        pl.when(core1)(functools.partial(left_first, 1))
        left_last()
        folds(of(6))
        left_sum(1)
        left_close()
        folds(of(7))
        step_rotate(0)
        rotate_own(0)
        folds(s.chunks)
        for k in range(1, s.kc):
            step_rotate(k)
            rotate_own(k)
        mids(of(6))
        rotated_all(0)
        mids(of(7))
        gather_all(0)
        mids(s.chunks)
        for k in range(1, s.kc):
            rotated_all(k)
            gather_all(k)

    def others():
        ends, folds, rests = upto(fold_end), upto(fold), upto(spread_rest)
        ends(of(4))
        step_old()
        step_new()
        left_ready()
        left_first(0)
        pl.when(core0)(functools.partial(left_first, 1))
        for k in range(s.kc):
            recv(y_mom[k])
            ends(of(6 + 2 * k))
            mom_both(k)
        ends(s.chunks)
        left_sum(0)
        rests(of(2))
        pl.when(core1)(functools.partial(left_first, 1))
        rests(of(4))
        left_last()
        folds(of(6))
        left_sum(1)
        left_close()
        step_rotate(0)
        rotate_own(0)
        for k in range(1, s.kc):
            step_rotate(k)
            rotate_own(k)
        rotated_all(0)
        rests(of(6))
        folds(s.chunks)
        gather_all(0)
        for k in range(1, s.kc):
            rotated_all(k)
        rests(s.chunks)
        for k in range(1, s.kc):
            gather_all(k)

    first_part()
    within(is_mid, middle)
    within(not_mid, others)
    order = [(h, n) for h in (1, 0) for n in range(0, s.chunks, s.wide)]
    seen = set()
    last = []
    for h, n in order:
        if not seen & {("rows", h)}:
            seen.add(("rows", h))
            for part in parts:
                if part[1] == h:
                    for d in range(s.nx):
                        recv(rot_c[d, part])
        for i in range(s.wide):
            if n + i not in seen:
                seen.add(n + i)
                recv(right_y[n + i])
        item = product(h, n)
        last.append((h, item))
    for h, item in last:
        (recv if h else done)(item)
    for copy, uses in drains.values():
        preds = []
        for pair in uses:
            terms = [term for term in pair if term is not None]
            preds.append(functools.reduce(jnp.logical_and, terms) if terms else None)
        sent(copy, None if any(p is None for p in preds) else functools.reduce(jnp.logical_or, preds))
    assert count[0] <= ssem.shape[0] and count[1] <= lsem.shape[0] - 3, count


def make_local(n_row, n_col):
    def local(moment, second, left_old, left_new, right_old, right_new):
        s = Sizes(n_row, n_col, left_old.shape, right_old.shape)
        rows2 = 2 * s.j
        any_spec = pl.BlockSpec(memory_space=pl.ANY)
        n_sems = 60 + 8 * s.chunks + 8 * s.classes * s.kc + 32 * s.nx * s.kc
        flops = 7 * 2 * (rows2 * s.nc * s.k * s.k) // 2
        moment_new, *_ = pl.pallas_call(
            functools.partial(kernel, s),
            out_shape=(
                jax.ShapeDtypeStruct(moment.shape, BF16),
                jax.ShapeDtypeStruct((s.w, s.j), BF16),
                jax.ShapeDtypeStruct((s.nc, 2, s.q, s.half), BF16),
                jax.ShapeDtypeStruct((s.chunks, s.nc * s.half, s.pc), BF16),
            ),
            in_specs=[any_spec] * 5,
            out_specs=(any_spec,) * 4,
            scratch_shapes=[
                pltpu.VMEM((2, 4, s.w, s.j), BF16),
                pltpu.VMEM((2, s.group, 2, s.w, s.j), BF16),
                pltpu.VMEM((s.classes, 2, s.j, s.k), BF16),
                pltpu.VMEM((2, s.q, s.k), BF16),
                pltpu.VMEM((2, s.q, s.half), BF16),
                pltpu.VMEM((s.chunks, s.nc * s.half, s.pc), BF16),
                pltpu.VMEM((s.chunks, s.nc * s.half, s.pc), BF16),
                pltpu.VMEM((s.chunks, 2, s.nc * s.half, s.pc), BF16),
                pltpu.VMEM((2, 2, rows2, s.cols), BF16),
                pltpu.VMEM((max(1, s.nx - 1), 2, rows2, s.cols), BF16),
                pltpu.VMEM((rows2, s.k), BF16),
                pltpu.VMEM((rows2, s.k), BF16),
                pltpu.VMEM((s.nc, rows2, s.k), BF16),
                pltpu.VMEM((s.nc * s.half, s.pc), BF16),
                pltpu.SemaphoreType.DMA((n_sems,)),
                pltpu.SemaphoreType.DMA((n_sems,)),
                pltpu.SemaphoreType.DMA((24,)),
            ],
            compiler_params=pltpu.CompilerParams(has_side_effects=True, collective_id=0, vmem_limit_bytes=67043328),
            cost_estimate=pl.CostEstimate(flops=flops, bytes_accessed=2**24, transcendentals=0),
        )(moment, left_old, left_new, right_old, right_new)
        direction = (moment_new.astype(F32) / (jnp.sqrt(second) + 1e-08)).astype(BF16)
        return moment_new, direction

    return local


def solution(mesh):
    spec = P(None, "row", "col")
    return jax.shard_map(
        make_local(mesh.shape["row"], mesh.shape["col"]),
        mesh=mesh,
        in_specs=(spec, spec, P(None, "col", "row"), P(None, "col", "row"), P("row", "col"), P("row", "col")),
        out_specs=(spec, spec),
        check_vma=False,
    )
```

```python
import functools

import jax
import jax.numpy as jnp
from jax import lax
from jax.experimental import pallas as pl
from jax.experimental.pallas import tpu as pltpu
from jax.sharding import PartitionSpec as P

F32 = jnp.float32
BF16 = jnp.bfloat16
MESH = pl.DeviceIdType.MESH


def dot_tn(a, b):
    return lax.dot_general(a, b, (((0,), (0,)), ((), ())), preferred_element_type=F32)


def dot(a, b):
    return jnp.dot(a, b, preferred_element_type=F32)


class Sizes:
    def __init__(self, n_row, n_col, left_shape, right_shape):
        self.nz, self.nx, self.nc = n_row // 2, n_col // 2, n_col
        self.classes = self.nz // 2
        self.group = self.classes // 2
        _, self.w, self.j = left_shape
        self.q, self.k = right_shape
        self.half = self.k // 2
        self.pc = 128
        self.chunks = self.k // self.pc
        self.wide = 2
        self.late = 1
        self.kc = 2
        self.kw = self.k // self.kc
        self.cols = self.group * 2 * self.j
        self.tile = min(256, self.j)


def kernel(s, mom, lo, ln, ro, rn, mo, yold, ro_all, fold_in, new, old, mm, rnv, ros, rp, cross, right, left, xrecv, buf, rot_in, rot_all, stage, ssem, rsem, lsem):
    row, col = lax.axis_index("row"), lax.axis_index("col")
    y, z = lax.rem(row, 2), lax.div(row, 2)
    c, x = lax.rem(col, 2), lax.div(col, 2)
    yp, cp = 1 - y, 1 - c
    zp = z + 1 - 2 * lax.rem(z, 2)
    depth = jnp.minimum(z, s.nz - 1 - z)
    upper = z >= s.nz // 2
    inner = jnp.where(upper, z - 1, z + 1)
    outer = jnp.where(upper, z + 1, z - 1)
    is_mid = depth == s.nz // 2 - 1
    is_end = depth == 0
    not_mid, not_end = jnp.logical_not(is_mid), jnp.logical_not(is_end)
    between, mid_out = not_mid & not_end, is_mid & not_end
    core0, core1 = c == 0, c == 1
    count = [0, 0]
    drains = {}
    branch = [None]

    def where_is(zz, yy, xx, cc):
        return (zz * 2 + yy, xx * 2 + cc)

    def fresh(n=1):
        count[0] += n
        return count[0] - n

    def remote(src, dst, target, sem):
        return pltpu.make_async_remote_copy(
            src_ref=src, dst_ref=dst, send_sem=ssem.at[sem], recv_sem=rsem.at[sem], device_id=target, device_id_type=MESH
        )

    def begin(copy, pred=None, drain=True):
        if pred is None:
            copy.start()
        else:
            pl.when(pred)(copy.start)
        if drain:
            drains.setdefault(id(copy), (copy, []))[1].append((branch[0], pred))

    def within(pred, fn):
        def run():
            branch[0] = pred
            fn()
            branch[0] = None
        pl.when(pred)(run)

    settled = set()

    def settle(keys):
        for key in keys:
            copy, uses = drains[key]
            for n, (where, pred) in enumerate(uses):
                if where is None or where is branch[0]:
                    sent(copy, pred)
                    settled.add((key, n))

    def recv(copy, pred=None):
        if pred is None:
            copy.wait_recv()
        else:
            pl.when(pred)(copy.wait_recv)

    def sent(copy, pred=None):
        if pred is None:
            copy.wait_send()
        else:
            pl.when(pred)(copy.wait_send)

    def load(src, dst, pred=None):
        count[1] += 1
        copy = pltpu.make_async_copy(src, dst, lsem.at[count[1] - 1])
        if pred is None:
            copy.start()
        else:
            pl.when(pred)(copy.start)
        return copy, pred

    def done(item):
        copy, pred = item
        if pred is None:
            copy.wait()
        else:
            pl.when(pred)(copy.wait)

    near_y = where_is(z, yp, x, c)
    near_c = where_is(z, y, x, cp)
    near_z = where_is(zp, y, x, c)

    def at_class(d, core):
        return where_is(lax.rem(z - 2 * d + s.nz, s.nz), y, x, core)

    def at_x(d):
        return where_is(z, y, lax.rem(x + d, s.nx), c)

    def col_from(d):
        return lax.rem(x - d + s.nx, s.nx) * 2 + c

    own_half = pl.ds(pl.multiple_of(y * s.half, s.half), s.half)
    other_half = pl.ds(pl.multiple_of(yp * s.half, s.half), s.half)

    loads_new = load(ln.at[y], new.at[c, 0])
    loads_old = [load(lo.at[y], old.at[0, 0, 0], c == 0), (pltpu.make_async_copy(yold, old.at[0, 0, 1], lsem.at[lsem.shape[0] - 3]), c == 0)]
    loads_rn = load(rn, rnv.at[0])
    loads_mom = load(mom.at[y], mm.at[0, 0])

    barrier = pltpu.get_barrier_semaphore()

    def greet(target):
        pl.semaphore_signal(barrier, inc=1, device_id=target, device_id_type=MESH)

    greet(near_y)
    greet(near_c)
    for d in range(1, s.nx):
        greet(at_x(d))
    for d in range(1, s.classes):
        for core in range(2):
            greet(at_class(d, core))
    pl.when(z > 0)(lambda: greet(where_is(z - 1, y, x, c)))
    pl.when(z < s.nz - 1)(lambda: greet(where_is(z + 1, y, x, c)))
    inside = jnp.where((z > 0) & (z < s.nz - 1), 2, 1)
    pl.semaphore_wait(barrier, 2 + s.nx - 1 + 2 * (s.classes - 1) + inside)

    y_ro = remote(ro.at[:, other_half], ro_all.at[col, 1], near_y, fresh())
    y_rn = remote(rn, rnv.at[1], near_y, fresh())
    y_old = remote(lo.at[yp], yold, near_y, fresh())
    y_new = remote(ln.at[yp], new.at[c, 1], near_y, fresh())
    y_mom = [remote(mom.at[yp, :, pl.ds(k * s.kw, s.kw)], mm.at[0, 1, :, pl.ds(k * s.kw, s.kw)], near_y, fresh()) for k in range(s.kc)]

    old_sems = {(d, p): fresh(2) for d in range(s.classes) for p in range(2)}

    def old_copy(d, p, who):
        src = lo.at[y] if p == 0 else yold
        return remote(src, old.at[who, d % s.group, p], at_class(d, d // s.group), old_sems[d, p] + who)

    old_far = {(d, p): old_copy(d, p, c) for d in range(1, s.classes) for p in range(2)}
    old_near = [old_copy(0, p, 1) for p in range(2)]
    new_z = [remote(ln.at[y] if p == 0 else new.at[c, 1], new.at[c, 2 + p], near_z, fresh()) for p in range(2)]
    new_c = [remote(ln.at[y] if p == 0 else new.at[c, p], new.at[c, p], near_c, fresh()) for p in range(4)]

    def mom_src(p, k):
        part = pl.ds(k * s.kw, s.kw)
        return mom.at[y, :, part] if p == 0 else mm.at[0, 1, :, part]

    mom_z = {
        (d, p, k): remote(mom_src(p, k), mm.at[d, p, :, pl.ds(k * s.kw, s.kw)], at_class(d, c), fresh())
        for d in range(1, s.classes) for p in range(2) for k in range(s.kc)
    }
    ro_src = [ro.at[:, own_half], ro_all.at[col, 1]]
    ro_c = {(0, p): remote(ro_src[p], ro_all.at[col, p], near_c, fresh()) for p in range(2)}
    ro_x = {(d, p): remote(ro_src[p], ro_all.at[col, p], at_x(d), fresh()) for d in range(1, s.nx) for p in range(2)}
    for d in range(1, s.nx):
        for p in range(2):
            ro_c[d, p] = remote(ro_all.at[col_from(d), p], ro_all.at[col_from(d), p], near_c, fresh())

    def old_send(d, p):
        if d == 0:
            begin(old_near[p], core1)
        else:
            begin(old_far[d, p])

    def mom_send(p, k, pred=None):
        for d in range(1, s.classes):
            begin(mom_z[d, p, k], pred)

    def step_start():
        begin(y_ro)
        begin(y_rn)
        begin(y_old)
        begin(y_new)
        for item in y_mom:
            begin(item)
        for d in range(1, s.classes):
            old_send(d, 0)
        begin(new_z[0])
        mom_send(0, 0, is_mid)
        begin(ro_c[0, 0])
        for d in range(1, s.nx):
            begin(ro_x[d, 0])
        begin(new_c[0])
        old_send(0, 0)

    def step_right_old():
        recv(y_ro)
        begin(ro_c[0, 1])
        for d in range(1, s.nx):
            begin(ro_x[d, 1])
        for d in range(1, s.nx):
            for p in range(2):
                recv(ro_x[d, p])
                begin(ro_c[d, p])

    steps = s.half // s.tile

    def stage_sem(n):
        return lsem.at[lsem.shape[0] - 1 - n]

    def right_piece(i, _):
        mine = i == col
        head = pltpu.make_async_copy(ro.at[:, own_half], ros.at[0], stage_sem(0))
        head_far = pltpu.make_async_copy(ro_all.at[i, 0], ros.at[0], stage_sem(0))
        tail = pltpu.make_async_copy(ro_all.at[i, 1], ros.at[1], stage_sem(1))
        pl.when(mine)(head.start)
        pl.when(jnp.logical_not(mine))(head_far.start)
        tail.start()
        head.wait()
        tail.wait()

        for t in range(steps):
            part = pl.ds(t * s.tile, s.tile)
            value = dot_tn(ros[0, :, part], rnv[0]) + dot_tn(ros[1, :, part], rnv[1])
            value = value.astype(BF16)
            rows = pl.ds(pl.multiple_of(i * s.half + t * s.tile, s.tile), s.tile)
            for n in range(s.chunks):
                rp[n, rows, :] = value[:, n * s.pc:(n + 1) * s.pc]
        return 0

    def step_right():
        recv(y_rn)
        done(loads_rn)
        for d in range(s.nx):
            for p in range(2):
                recv(ro_c[d, p])
        lax.fori_loop(0, s.nc, right_piece, 0)

    fold_send = [remote(rp.at[n], fold_in.at[n], where_is(inner, y, x, c), fresh()) for n in range(s.chunks)]
    cross_send = [remote(rp.at[n], cross.at[n], where_is(inner, y, x, c), fresh()) for n in range(s.chunks)]
    out_send = [remote(right.at[n, y], right.at[n, y], where_is(outer, y, x, c), fresh()) for n in range(s.chunks)]
    right_y = [remote(right.at[n, y], right.at[n, y], near_y, fresh()) for n in range(s.chunks)]
    late = range(s.chunks - s.late, s.chunks)
    out_far = {n: remote(right.at[n, yp], right.at[n, yp], where_is(outer, y, x, c), fresh()) for n in late}
    total_rows = s.nc * s.half
    part_rows = min(256, total_rows)

    def over_rows(fn):
        def step(i, _):
            fn(pl.ds(pl.multiple_of(i * part_rows, part_rows), part_rows))
            return 0
        lax.fori_loop(0, total_rows // part_rows, step, 0)

    def fold_end(n):
        begin(fold_send[n], is_end)

    def fold(n):
        @pl.when(not_end)
        def _():
            fold_send[n].wait_recv()
            copy = pltpu.make_async_copy(fold_in.at[n], stage, stage_sem(0))
            copy.start()
            copy.wait()

            def step(rows):
                rp[n, rows, :] = (rp[n, rows, :].astype(F32) + stage[rows, :].astype(F32)).astype(BF16)
            over_rows(step)

        begin(fold_send[n], between)
        begin(cross_send[n], is_mid)

    def spread_mid(n):
        @pl.when(is_mid)
        def _():
            cross_send[n].wait_recv()

            def step(rows):
                right[n, y, rows, :] = (rp[n, rows, :].astype(F32) + cross[n, rows, :].astype(F32)).astype(BF16)
            over_rows(step)

        begin(out_send[n], mid_out)
        begin(right_y[n], is_mid)

    def spread_rest(n):
        recv(out_send[n], not_mid)
        begin(out_send[n], between)
        if n not in late:
            begin(right_y[n], not_mid)

    def step_old():
        recv(y_old)
        for d in range(1, s.classes):
            old_send(d, 1)
        old_send(0, 1)
        loads_old[1][0].start() if loads_old[1][1] is None else pl.when(loads_old[1][1])(loads_old[1][0].start)

    def step_new():
        recv(y_new)
        begin(new_z[1])
        begin(new_c[1])

    def step_mom(k):
        recv(y_mom[k])
        mom_send(1, k)

    per = s.j // s.tile

    def left_rows(piece, p):
        h = piece // 2

        def step(t, _):
            lanes = pl.ds(pl.multiple_of(t * s.tile, s.tile), s.tile)
            rows = pl.ds(pl.multiple_of((piece % 2) * s.j + t * s.tile, s.tile), s.tile)
            first = jnp.transpose(new[0, piece, :, lanes])
            second = jnp.transpose(new[1, piece, :, lanes])
            for d in range(s.group):
                value = dot(first, old[0, d, p]) + dot(second, old[1, d, p])
                left[c, h, rows, pl.ds((p * s.group + d) * s.j, s.j)] = value.astype(BF16)
            return 0
        lax.fori_loop(0, per, step, 0)

    half_cols = s.cols // 2

    def left_part(ref, index, piece, p):
        return ref.at[index, piece // 2, pl.ds((piece % 2) * s.j, s.j), pl.ds(p * half_cols, half_cols)]

    left_units = [(i, p) for p in range(2) for i in (2, 0, 1, 3)]
    left_x = {
        (d,) + u: remote(left_part(left, c, *u), left_part(xrecv, d - 1, *u), at_x(d), fresh())
        for d in range(1, s.nx) for u in left_units
    }
    left_c = {u: remote(left_part(left, c, *u), left_part(left, c, *u), near_c, fresh()) for u in left_units}

    def left_send(piece, p):
        left_rows(piece, p)
        for d in range(1, s.nx):
            begin(left_x[d, piece, p], drain=False)

    def left_first(p):
        for d in range(s.classes):
            g = d // s.group
            for who in range(2):
                if d == 0 and who == 0:
                    done(loads_old[p])
                else:
                    recv(old_copy(d, p, who), c == g)
        for i in (2, 0, 1):
            left_send(i, p)

    def left_total(piece, p):
        for d in range(1, s.nx):
            left_x[d, piece, p].wait()
        lanes = pl.ds(p * half_cols, half_cols)

        def step(t, _):
            rows = pl.ds(pl.multiple_of((piece % 2) * s.j + t * s.tile, s.tile), s.tile)
            value = left[c, piece // 2, rows, lanes].astype(F32)
            for d in range(1, s.nx):
                value = value + xrecv[d - 1, piece // 2, rows, lanes].astype(F32)
            left[c, piece // 2, rows, lanes] = value.astype(BF16)
            return 0
        lax.fori_loop(0, per, step, 0)
        begin(left_c[piece, p])

    rows2 = 2 * s.j
    parts = [(k, h) for k in range(s.kc) for h in (1, 0)]

    def cut(part):
        k, h = part
        return pl.ds(h * s.j, s.j), pl.ds(k * s.kw, s.kw)

    rot_z = {part: remote(buf.at[cut(part)], rot_in.at[cut(part)], near_z, fresh()) for part in parts}

    def rot_part(cc, part):
        return rot_all.at[(cc,) + cut(part)]

    rot_c = {(0, part): remote(rot_part(col, part), rot_part(col, part), near_c, fresh()) for part in parts}
    rot_x = {}
    for d in range(1, s.nx):
        for part in parts:
            rot_x[d, part] = remote(rot_part(col, part), rot_part(col, part), at_x(d), fresh())
            rot_c[d, part] = remote(rot_part(col_from(d), part), rot_part(col_from(d), part), near_c, fresh())

    def over_half(h, fn):
        def step(i, _):
            fn(pl.ds(pl.multiple_of(h * s.j + i * s.tile, s.tile), s.tile))
            return 0
        lax.fori_loop(0, per, step, 0)

    def rotate(h, part, put):
        lanes = cut(part)[1]

        def step(rows):
            value = None
            for g in range(2):
                for d in range(s.group):
                    for p in range(2):
                        term = dot(left[g, h, rows, pl.ds((p * s.group + d) * s.j, s.j)], mm[g * s.group + d, p, :, lanes])
                        value = term if value is None else value + term
            put(rows, lanes, value)
        over_half(part[1], step)

    def put_far(rows, lanes, value):
        buf[rows, lanes] = value.astype(BF16)

    def put_own(rows, lanes, value):
        rot_all[col, rows, lanes] = value.astype(BF16)

    def step_rotate(k):
        for p in range(2):
            for d in range(1, s.classes):
                recv(mom_z[d, p, k])
        for h in (1, 0):
            rotate(1, (k, h), put_far)
            begin(rot_z[k, h], drain=False)

    def step_rotated(part):
        lanes = cut(part)[1]
        rot_z[part].wait()

        def step(rows):
            rot_all[col, rows, lanes] = (rot_all[col, rows, lanes].astype(F32) + rot_in[rows, lanes].astype(F32)).astype(BF16)
        over_half(part[1], step)
        for d in range(1, s.nx):
            begin(rot_x[d, part])
        begin(rot_c[0, part])

    def step_gather(part):
        for d in range(1, s.nx):
            recv(rot_x[d, part])
            begin(rot_c[d, part])

    def product(h, n):
        lanes = pl.ds(n * s.pc, s.wide * s.pc)

        def step(rows):
            value = None
            for piece in range(s.nc):
                for i in range(2):
                    deep = pl.ds(piece * s.half, s.half)
                    columns = jnp.concatenate([right[n + j, i, deep, :] for j in range(s.wide)], axis=1)
                    term = dot(rot_all[piece, rows, pl.ds(i * s.half, s.half)], columns)
                    value = term if value is None else value + term
            buf[rows, lanes] = value.astype(BF16)
        over_half(h, step)
        if h:
            far = remote(buf.at[pl.ds(s.j, s.j), lanes], mo.at[y, :, lanes], near_y, fresh())
            begin(far)
            return far
        return load(buf.at[pl.ds(0, s.j), lanes], mo.at[y, :, lanes])

    def upto(step):
        state = [0]

        def run(n):
            while state[0] < min(n, s.chunks):
                step(state[0])
                state[0] += 1
        return run

    ends, folds, mids, rests = upto(fold_end), upto(fold), upto(spread_mid), upto(spread_rest)
    eighth = max(1, s.chunks // 8)

    def first_part():
        step_start()
        step_right_old()
        step_right()

    def left_ready():
        done(loads_new)
        recv(new_z[0])
        begin(new_c[2])
        for i in range(3):
            recv(new_c[i])

    def left_last():
        recv(new_z[1])
        begin(new_c[3])
        recv(new_c[3])
        for p in range(2):
            left_send(3, p)

    def left_sum(p):
        for i in (2, 0, 1):
            left_total(i, p)

    def left_close():
        for p in range(2):
            left_total(3, p)
        done(loads_mom)
        for u in left_units:
            recv(left_c[u])

    def rotate_own(k):
        for h in (1, 0):
            rotate(0, (k, h), put_own)

    def rotated_all(k):
        for h in (1, 0):
            step_rotated((k, h))

    def gather_all(k):
        for h in (1, 0):
            step_gather((k, h))

    def mom_both(k):
        mom_send(0, k, not_mid if k == 0 else None)
        mom_send(1, k)

    def of(n):
        return max(1, n * s.chunks // 8)

    def middle():
        folds, mids = upto(fold), upto(spread_mid)
        folds(of(2))
        mids(of(1))
        folds(of(3))
        step_new()
        mids(of(2))
        folds(of(4))
        step_old()
        left_ready()
        left_first(0)
        mids(of(3))
        pl.when(core0)(functools.partial(left_first, 1))
        for k in range(s.kc):
            recv(y_mom[k])
        mids(of(4))
        for k in range(s.kc):
            mom_both(k)
        left_sum(0)
        pl.when(core1)(functools.partial(left_first, 1))
        left_last()
        folds(of(6))
        left_sum(1)
        left_close()
        early = list(drains)
        folds(of(7))
        step_rotate(0)
        rotate_own(0)
        folds(s.chunks)
        for k in range(1, s.kc):
            step_rotate(k)
            rotate_own(k)
        mids(of(5))
        rotated_all(0)
        mids(of(6))
        settle(early)
        recent = [key for key in drains if key not in early]
        mids(of(7))
        for k in range(1, s.kc):
            rotated_all(k)
        mids(s.chunks)
        for k in range(s.kc - 1):
            gather_all(k)
        settle(recent)
        for n in late:
            recv(right_y[n])
            begin(out_far[n], mid_out)
        gather_all(s.kc - 1)

    def others():
        ends, folds, rests = upto(fold_end), upto(fold), upto(spread_rest)
        ends(of(4))
        step_old()
        step_new()
        left_ready()
        left_first(0)
        pl.when(core0)(functools.partial(left_first, 1))
        for k in range(s.kc):
            recv(y_mom[k])
            ends(of(6 + 2 * k))
            mom_both(k)
        ends(s.chunks)
        left_sum(0)
        rests(of(2))
        pl.when(core1)(functools.partial(left_first, 1))
        rests(of(4))
        left_last()
        folds(of(6))
        left_sum(1)
        left_close()
        early = list(drains)
        step_rotate(0)
        rotate_own(0)
        for k in range(1, s.kc):
            step_rotate(k)
            rotate_own(k)
        rotated_all(0)
        rests(of(5))
        for k in range(1, s.kc):
            rotated_all(k)
        gather_all(0)
        rests(of(6))
        folds(s.chunks)
        recent = [key for key in drains if key not in early]
        rests(s.chunks)
        settle(early)
        for k in range(1, s.kc):
            gather_all(k)
        settle(recent)

    first_part()
    within(is_mid, middle)
    within(not_mid, others)
    order = [(h, n) for h in (1, 0) for n in range(0, s.chunks, s.wide)]
    seen = set()
    last = []
    for h, n in order:
        if not seen & {("rows", h)}:
            seen.add(("rows", h))
            for part in parts:
                if part[1] == h:
                    for d in range(s.nx):
                        recv(rot_c[d, part])
        for i in range(s.wide):
            if n + i not in seen:
                seen.add(n + i)
                if n + i not in late:
                    recv(right_y[n + i])
                else:
                    recv(out_far[n + i], not_mid)
                    begin(out_far[n + i], between)
        item = product(h, n)
        last.append((h, item))
    for h, item in last:
        (recv if h else done)(item)
    for key, (copy, uses) in drains.items():
        uses = [use for n, use in enumerate(uses) if (key, n) not in settled]
        preds = [[term for term in use if term is not None] for use in uses]
        if any(not terms for terms in preds):
            sent(copy)
        elif preds:
            sent(copy, functools.reduce(jnp.logical_or, [functools.reduce(jnp.logical_and, terms) for terms in preds]))
    assert count[0] <= ssem.shape[0] and count[1] <= lsem.shape[0] - 3, count


def make_local(n_row, n_col):
    def local(moment, second, left_old, left_new, right_old, right_new):
        s = Sizes(n_row, n_col, left_old.shape, right_old.shape)
        rows2 = 2 * s.j
        any_spec = pl.BlockSpec(memory_space=pl.ANY)
        n_sems = 60 + 8 * s.chunks + 8 * s.classes * s.kc + 32 * s.nx * s.kc
        flops = 7 * 2 * (rows2 * s.nc * s.k * s.k) // 2
        moment_new, *_ = pl.pallas_call(
            functools.partial(kernel, s),
            out_shape=(
                jax.ShapeDtypeStruct(moment.shape, BF16),
                jax.ShapeDtypeStruct((s.w, s.j), BF16),
                jax.ShapeDtypeStruct((s.nc, 2, s.q, s.half), BF16),
                jax.ShapeDtypeStruct((s.chunks, s.nc * s.half, s.pc), BF16),
            ),
            in_specs=[any_spec] * 5,
            out_specs=(any_spec,) * 4,
            scratch_shapes=[
                pltpu.VMEM((2, 4, s.w, s.j), BF16),
                pltpu.VMEM((2, s.group, 2, s.w, s.j), BF16),
                pltpu.VMEM((s.classes, 2, s.j, s.k), BF16),
                pltpu.VMEM((2, s.q, s.k), BF16),
                pltpu.VMEM((2, s.q, s.half), BF16),
                pltpu.VMEM((s.chunks, s.nc * s.half, s.pc), BF16),
                pltpu.VMEM((s.chunks, s.nc * s.half, s.pc), BF16),
                pltpu.VMEM((s.chunks, 2, s.nc * s.half, s.pc), BF16),
                pltpu.VMEM((2, 2, rows2, s.cols), BF16),
                pltpu.VMEM((max(1, s.nx - 1), 2, rows2, s.cols), BF16),
                pltpu.VMEM((rows2, s.k), BF16),
                pltpu.VMEM((rows2, s.k), BF16),
                pltpu.VMEM((s.nc, rows2, s.k), BF16),
                pltpu.VMEM((s.nc * s.half, s.pc), BF16),
                pltpu.SemaphoreType.DMA((n_sems,)),
                pltpu.SemaphoreType.DMA((n_sems,)),
                pltpu.SemaphoreType.DMA((24,)),
            ],
            compiler_params=pltpu.CompilerParams(has_side_effects=True, collective_id=0, vmem_limit_bytes=67043328),
            cost_estimate=pl.CostEstimate(flops=flops, bytes_accessed=2**24, transcendentals=0),
        )(moment, left_old, left_new, right_old, right_new)
        direction = (moment_new.astype(F32) / (jnp.sqrt(second) + 1e-08)).astype(BF16)
        return moment_new, direction

    return local


def solution(mesh):
    spec = P(None, "row", "col")
    return jax.shard_map(
        make_local(mesh.shape["row"], mesh.shape["col"]),
        mesh=mesh,
        in_specs=(spec, spec, P(None, "col", "row"), P(None, "col", "row"), P("row", "col"), P("row", "col")),
        out_specs=(spec, spec),
        check_vma=False,
    )
```
